128 devices in a mesh: head: 4 (over y_hi, core), seq: 32 (over x, z, y_lo).
Axes of the slice: x: 4, y: 4 (y_hi: 2, y_lo: 2; y = y_hi * 2 + y_lo), z: 4, core: 2. Of those that a mesh axis runs over, the one named last changes fastest.
Arguments:
- queries: bfloat16 [32768, 4096], P('seq', 'head'), may hold values from -6 to 6
- keys: bfloat16 [32768, 512], P('seq', 'head'), may hold values from -6 to 6
- values: bfloat16 [32768, 512], P('seq', 'head'), may hold values from -6 to 6
- vertical: int32 [32, 8], P('head'), may hold values from 0 to 255, as said below
- slash: int32 [32, 8], P('head'), may hold values from 1 to 28, as said below
Outputs:
- attended: bfloat16 [32768, 4096], P(('seq', 'head'))
The draws below stay inside these ranges and needn't reach their ends.
Inputs may be any that keep to these rules, and one draw needn't show every extreme that they name: `vertical`: each row names 8 different blocks. Within each group of 8 consecutive rows, the different blocks named that lie in one slab (blocks s * 8 to s * 8 + 7) number at most 4, and exactly 4 in some slab. `slash`: each row names 8 different offsets.
All inputs are finite; a program needn't handle non-finite values.
Results may differ from the reference program's by a relative error of at most 0.0033.
Values may be sent and summed in bfloat16 or wider, within the bound.
No kernel may reach another device: no remote copies, remote signals or barrier semaphores. Data moves between devices by JAX's collectives and lax.ppermute only.
A program may use at most 128 MiB of HBM per device.

```python
import math
import jax
import jax.numpy as jnp
from jax import lax

HD = 128
QUERY_PER_GROUP = 8
BLK = 128
VERTICAL_BLOCKS = 8
SLASH_OFFSETS = 8
LARGEST_OFFSET = 28
CAP = 4
GROUPS = 4
HEADS = 32
BLK_DEV = 8
SLABS = 32
SEQ = 32768
BLOCKS = 256


def draw_queries(key, part):
    own_key = jax.random.fold_in(key, 11)
    drawn = jnp.clip(1.5 * jax.random.normal(own_key, (SEQ, GROUPS, QUERY_PER_GROUP, HD), jnp.float32), -6.0, 6.0)
    return drawn.reshape(SEQ, HEADS * HD).astype(jnp.bfloat16)


def draw_keys(key, part):
    own_key = jax.random.fold_in(key, 12)
    drawn = jnp.clip(1.5 * jax.random.normal(own_key, (SEQ, GROUPS, HD), jnp.float32), -6.0, 6.0)
    return drawn.reshape(SEQ, GROUPS * HD).astype(jnp.bfloat16)


def vertical_group(key):
    key_count, key_full, key_order, key_pick = jax.random.split(key, 4)
    slab_ids = jnp.arange(SLABS, dtype=jnp.int32)
    counts = jax.random.randint(key_count, (SLABS,), 1, CAP + 1)
    fullest = jax.random.randint(key_full, (), 0, SLABS)
    counts = jnp.where(slab_ids == fullest, CAP, counts)
    order_scores = jax.random.randint(key_order, (SLABS, BLK_DEV), 0, 4096) * BLK_DEV + jnp.arange(BLK_DEV, dtype=jnp.int32)[None, :]
    ranks = jnp.argsort(jnp.argsort(order_scores, axis=1), axis=1)
    inside = ranks < counts[:, None]
    mandatory_blocks = (inside & (slab_ids[:, None] == fullest)).reshape(BLOCKS)
    inside = inside.reshape(BLOCKS)
    selected_indices = jax.random.randint(key_pick, (QUERY_PER_GROUP, BLOCKS), 0, 65536) * BLOCKS + jnp.arange(BLOCKS, dtype=jnp.int32)[None, :] + 1
    selected_indices = jnp.where(inside[None, :], selected_indices, 0)
    extra_score = jnp.where((jnp.arange(QUERY_PER_GROUP)[:, None] == 0) & mandatory_blocks[None, :], 1 << 29, 0)
    leftover_slots, selected_blocks = lax.top_k(selected_indices + extra_score, VERTICAL_BLOCKS)
    return selected_blocks.astype(jnp.int32)


def draw_vertical(key, part):
    group_keys = jax.random.split(jax.random.fold_in(key, 31), GROUPS)
    return jax.vmap(vertical_group)(group_keys).reshape(HEADS, VERTICAL_BLOCKS).astype(jnp.int32)


def draw_slash(key, part):
    block_scores = jax.random.randint(jax.random.fold_in(key, 41), (HEADS, LARGEST_OFFSET), 0, 65536) * LARGEST_OFFSET + jnp.arange(LARGEST_OFFSET, dtype=jnp.int32)[None, :] + 1
    per_head_rows = jnp.arange(HEADS)[:, None]
    offset_columns = jnp.arange(LARGEST_OFFSET)[None, :]
    extra_score = jnp.where((per_head_rows == 0) & (offset_columns == LARGEST_OFFSET - 1), 1 << 28, 0)
    extra_score = extra_score + jnp.where((per_head_rows == 1) & (offset_columns == 0), 1 << 28, 0)
    leftover_slots, selected_blocks = lax.top_k(block_scores + extra_score, SLASH_OFFSETS)
    return (selected_blocks + 1).astype(jnp.int32)


def block_levels(key, extent, pieces, least, largest):
    factor_of, own = 1.0, jax.random.fold_in(key, 6)
    for position, shards_of in pieces:
        steps = jnp.exp(jax.random.uniform(jax.random.fold_in(own, position), (shards_of,), jnp.float32, least / len(pieces), largest / len(pieces)))
        factor_of = factor_of * jnp.repeat(steps, extent[position] // shards_of).reshape([-1 if axis == position else 1 for axis in range(len(extent))])
    return factor_of


def normal_values(rng, dims, scale, limit, cuts=(), held_as=jnp.bfloat16):
    level = block_levels(rng, dims, cuts, -0.22, 0.18) if cuts else 1.0
    values = jax.random.normal(rng, dims, jnp.float32) * scale * level
    return jnp.minimum(jnp.maximum(values, -limit), limit).astype(held_as)


def setup_inputs(seed: int = 0) -> dict:
    key_list = jax.random.split(jax.random.key(seed), 6)
    return {
        "queries": draw_queries(jax.random.fold_in(key_list[5], 71), 0),
        "keys": draw_keys(jax.random.fold_in(key_list[5], 71), 0),
        "values": normal_values(key_list[2], (SEQ, GROUPS * HD), 1.0, 6.0, ((0, 32), (1, 4))),
        "vertical": draw_vertical(jax.random.fold_in(key_list[5], 71), 0),
        "slash": draw_slash(jax.random.fold_in(key_list[5], 71), 0),
    }


NEG = -1e+30

def attend(query_block, diag_kv, slash_kv, column_kv, slash_ok, column_ok):
    block_count, block_width, head_width = query_block.shape
    slash_count = slash_kv.shape[1]
    column_count = column_kv.shape[0]
    score_scale = 1.0 / math.sqrt(head_width)
    causal = jnp.arange(block_width)[:, None] >= jnp.arange(block_width)[None, :]
    diag_scores = jnp.einsum('ird,icd->irc', query_block, diag_kv[..., :head_width]) * score_scale
    diag_scores = jnp.where(causal[None], diag_scores, NEG)
    slash_scores = jnp.einsum('ird,ijcd->irjc', query_block, slash_kv[..., :head_width]) * score_scale
    slash_scores = jnp.where(slash_ok[:, None, :, None], slash_scores, NEG).reshape(block_count, block_width, slash_count * block_width)
    column_scores = jnp.einsum('ird,jcd->irjc', query_block, column_kv[..., :head_width]) * score_scale
    column_scores = jnp.where(column_ok[:, None, :, None], column_scores, NEG).reshape(block_count, block_width, column_count * block_width)
    block_scores = jnp.concatenate([diag_scores, slash_scores, column_scores], axis=2)
    row_top = lax.optimization_barrier(jnp.max(block_scores, axis=2, keepdims=True))
    weights = jnp.exp(block_scores - row_top)
    row_total = lax.optimization_barrier(jnp.sum(weights, axis=2))
    rounded = lax.optimization_barrier(weights.astype(jnp.bfloat16)).astype(jnp.float32)
    split_one = block_width
    split_two = block_width + slash_count * block_width
    w_diag = rounded[:, :, :split_one]
    w_slash = rounded[:, :, split_one:split_two].reshape(block_count, block_width, slash_count, block_width)
    w_column = rounded[:, :, split_two:].reshape(block_count, block_width, column_count, block_width)
    mixed_sum = jnp.einsum('irc,icd->ird', w_diag, diag_kv[..., head_width:])
    mixed_sum = mixed_sum + jnp.einsum('irjc,ijcd->ird', w_slash, slash_kv[..., head_width:])
    mixed_sum = mixed_sum + jnp.einsum('irjc,jcd->ird', w_column, column_kv[..., head_width:])
    return (mixed_sum / row_total[:, :, None]).astype(jnp.bfloat16)

def reference(queries, keys, values, vertical, slash):
    seq_rows = queries.shape[0]
    block_total = seq_rows // BLK
    joined = jnp.concatenate([keys.reshape(seq_rows, GROUPS, HD), values.reshape(seq_rows, GROUPS, HD)], axis=2)
    block_ids = jnp.arange(block_total, dtype=jnp.int32)

    def one_head(head_index):
        group_index = head_index // QUERY_PER_GROUP
        query_block = lax.dynamic_slice_in_dim(queries, head_index * HD, HD, 1).astype(jnp.float32).reshape(block_total, BLK, HD)
        group_kv = lax.dynamic_index_in_dim(joined, group_index, 1, keepdims=False).astype(jnp.float32).reshape(block_total, BLK, 2 * HD)
        padded = jnp.concatenate([jnp.zeros((LARGEST_OFFSET, BLK, 2 * HD), jnp.float32), group_kv], axis=0)
        offsets = lax.dynamic_index_in_dim(slash, head_index, 0, keepdims=False)
        columns = lax.dynamic_index_in_dim(vertical, head_index, 0, keepdims=False)
        slash_index = (LARGEST_OFFSET + block_ids[:, None] - offsets[None, :]).astype(jnp.int32)
        slash_kv = jnp.take(padded, slash_index, axis=0)
        slash_ok = block_ids[:, None] - offsets[None, :] >= 0
        column_kv = jnp.take(group_kv, columns.astype(jnp.int32), axis=0)
        covered = jnp.any(block_ids[:, None, None] - columns[None, :, None] == offsets[None, None, :], axis=2)
        column_ok = (columns[None, :] < block_ids[:, None]) & jnp.logical_not(covered)
        return attend(query_block, group_kv, slash_kv, column_kv, slash_ok, column_ok)
    outputs = lax.map(one_head, jnp.arange(HEADS, dtype=jnp.int32))
    return jnp.transpose(outputs, (1, 2, 0, 3)).reshape(seq_rows, HEADS * HD)
```

```python
import functools
import math

import jax
import jax.numpy as jnp
from jax import lax
from jax.experimental import pallas as pl
from jax.experimental.pallas import tpu as pltpu
from jax.sharding import Mesh
from jax.sharding import PartitionSpec as P

BLK = 128
HD = 128
REACH = 28
CAP = 4
NEG = -1e30
SEQ = ("x", "z", "y")
SCALE2 = math.log2(math.e) / math.sqrt(HD)


def prep_kernel(flat_ref, base_ref, keys_ref, values_ref, kv_ref, packed_ref):
    slab_blocks = kv_ref.shape[0]
    base = base_ref[0]

    def mark(entry, bits):
        local = flat_ref[entry] - base
        inside = (local >= 0) & (local < slab_blocks)
        return bits | jnp.where(inside, 1 << jnp.where(inside, local, 0), 0)

    bits = lax.fori_loop(0, flat_ref.shape[0], mark, jnp.int32(0))
    packed_ref[...] = jnp.zeros(packed_ref.shape, packed_ref.dtype)
    rank = jnp.int32(0)
    for block in range(slab_blocks):
        rows = pl.ds(block * BLK, BLK)
        kv_ref[block, :BLK, :] = keys_ref[rows, :].T
        kv_ref[block, BLK:, :] = values_ref[rows, :]
        used = (bits >> block) & 1

        @pl.when((used == 1) & (rank < CAP))
        def _(block=block, rank=rank):
            packed_ref[rank] = kv_ref[block]

        rank = rank + used


def prep(flat, base, keys, values):
    slab_blocks = keys.shape[0] // BLK
    whole = lambda shape: pl.BlockSpec(shape, lambda *_: (0,) * len(shape))
    return pl.pallas_call(
        prep_kernel,
        grid_spec=pltpu.PrefetchScalarGridSpec(
            num_scalar_prefetch=2,
            grid=(1,),
            in_specs=[whole(keys.shape), whole(values.shape)],
            out_specs=[whole((slab_blocks, 2 * BLK, HD)), whole((CAP, 2 * BLK, HD))],
        ),
        out_shape=[
            jax.ShapeDtypeStruct((slab_blocks, 2 * BLK, HD), jnp.bfloat16),
            jax.ShapeDtypeStruct((CAP, 2 * BLK, HD), jnp.bfloat16),
        ],
        name="prep",
    )(flat, base, keys, values)


def near_kernel(slash_ref, base_ref, q_ref, far_ref, third_ref, second_ref, first_ref, own_ref, acc_ref, stat_ref, band, sems):
    head = pl.program_id(0)
    slab_blocks = own_ref.shape[0]
    slash_count = slash_ref.shape[0] // pl.num_programs(0)

    @pl.when(head == 0)
    def _():
        start = 0
        copies = []
        for number, part in enumerate((far_ref, third_ref, second_ref, first_ref, own_ref)):
            copies.append(pltpu.make_async_copy(part, band.at[pl.ds(start, part.shape[0])], sems.at[number]))
            start += part.shape[0]
        for copy in copies:
            copy.start()
        for copy in copies:
            copy.wait()

    lanes = lax.broadcasted_iota(jnp.int32, (BLK, HD), 1)
    causal = lax.broadcasted_iota(jnp.int32, (BLK, BLK), 0) >= lanes
    base = base_ref[0]

    def one(index, _):
        rows = pl.ds(pl.multiple_of(index * BLK, BLK), BLK)
        q = q_ref[rows, :]
        offsets = [slash_ref[head * slash_count + n] for n in range(slash_count)]
        places = [index + REACH] + [index + REACH - s for s in offsets]
        kt = jnp.concatenate([band[p, :BLK, :] for p in places], axis=1)
        scores = jnp.dot(q, kt, preferred_element_type=jnp.float32)
        parts = [jnp.where(causal, scores[:, :BLK] * SCALE2, NEG)]
        for n, s in enumerate(offsets):
            bias = jnp.where(base + index - s >= 0, 0.0, NEG).astype(jnp.float32)
            parts.append(scores[:, (n + 1) * BLK : (n + 2) * BLK] * SCALE2 + bias)
        top = functools.reduce(jnp.maximum, parts)
        top = jnp.max(top, axis=1, keepdims=True)
        weights = [jnp.exp2(p - top) for p in parts]
        total = jnp.sum(functools.reduce(jnp.add, weights), axis=1, keepdims=True)
        rounded = jnp.concatenate([w.astype(jnp.bfloat16) for w in weights], axis=1)
        v = jnp.concatenate([band[p, BLK:, :] for p in places], axis=0)
        acc_ref[rows, :] = jnp.dot(rounded, v, preferred_element_type=jnp.float32)
        old = stat_ref[rows, :]
        stat_ref[rows, :] = jnp.where(lanes == 2 * head, top, jnp.where(lanes == 2 * head + 1, total, old))
        return 0

    lax.fori_loop(0, slab_blocks, one, 0, unroll=2)


def near(slash, base, queries, far, third, second, first, own):
    rows, width = queries.shape
    heads = width // HD
    slab_blocks = rows // BLK
    hbm = pl.BlockSpec(memory_space=pl.ANY)
    return pl.pallas_call(
        near_kernel,
        grid_spec=pltpu.PrefetchScalarGridSpec(
            num_scalar_prefetch=2,
            grid=(heads,),
            in_specs=[pl.BlockSpec((rows, HD), lambda h, *_: (0, h))] + [hbm] * 5,
            out_specs=[
                pl.BlockSpec((rows, HD), lambda h, *_: (0, h)),
                pl.BlockSpec((rows, HD), lambda h, *_: (0, 0)),
            ],
            scratch_shapes=[
                pltpu.VMEM((REACH + slab_blocks, 2 * BLK, HD), jnp.bfloat16),
                pltpu.SemaphoreType.DMA((5,)),
            ],
        ),
        out_shape=[
            jax.ShapeDtypeStruct((rows, width), jnp.float32),
            jax.ShapeDtypeStruct((rows, HD), jnp.float32),
        ],
        compiler_params=pltpu.CompilerParams(dimension_semantics=("arbitrary",)),
        name="near",
    )(slash, base, queries, far, third, second, first, own)


def vertical_kernel(slab_blocks, slot_ref, ok_ref, quarter_ref, q_ref, acc_ref, stat_ref, *rest):
    columns, out_ref = rest[:-1], rest[-1]
    head = pl.program_id(0)
    count = len(columns)
    blocks = q_ref.shape[0] // BLK
    lanes = lax.broadcasted_iota(jnp.int32, (BLK, HD), 1)
    kt = jnp.concatenate([c[0, :BLK, :] for c in columns], axis=1)
    v = jnp.concatenate([c[0, BLK:, :] for c in columns], axis=0)
    for index in range(blocks):
        rows = pl.ds(index * BLK, BLK)
        where_ok = (head * slab_blocks + quarter_ref[0] * blocks + index) * count
        scores = jnp.dot(q_ref[rows, :], kt, preferred_element_type=jnp.float32)
        parts = []
        for k in range(count):
            bias = jnp.where(ok_ref[where_ok + k] > 0, 0.0, NEG).astype(jnp.float32)
            parts.append(scores[:, k * BLK : (k + 1) * BLK] * SCALE2 + bias)
        stat = stat_ref[rows, :]
        near_top = jnp.sum(jnp.where(lanes == 2 * head, stat, 0.0), axis=1, keepdims=True)
        near_total = jnp.sum(jnp.where(lanes == 2 * head + 1, stat, 0.0), axis=1, keepdims=True)
        top = jnp.max(functools.reduce(jnp.maximum, parts), axis=1, keepdims=True)
        top = jnp.maximum(top, near_top)
        weights = [jnp.exp2(p - top) for p in parts]
        total = jnp.sum(functools.reduce(jnp.add, weights), axis=1, keepdims=True)
        rounded = jnp.concatenate([w.astype(jnp.bfloat16) for w in weights], axis=1)
        far = jnp.dot(rounded, v, preferred_element_type=jnp.float32)
        shrink = jnp.exp2(near_top - top)
        out_ref[rows, :] = ((acc_ref[rows, :] * shrink + far) / (near_total * shrink + total)).astype(out_ref.dtype)


def vertical_part(slots, ok, quarter, queries, acc, stat, gathered, parts):
    rows, width = queries.shape
    heads = width // HD
    count = slots.shape[0] // heads
    part = rows // parts

    def column(k):
        return pl.BlockSpec((1, 2 * BLK, HD), lambda h, slot, ok, quarter: (slot[h * count + k], 0, 0))

    def mine(h, slot, ok, quarter):
        return quarter[0], h

    return pl.pallas_call(
        functools.partial(vertical_kernel, rows // BLK),
        grid_spec=pltpu.PrefetchScalarGridSpec(
            num_scalar_prefetch=3,
            grid=(heads,),
            in_specs=[
                pl.BlockSpec((part, HD), mine),
                pl.BlockSpec((part, HD), mine),
                pl.BlockSpec((part, HD), lambda h, slot, ok, quarter: (quarter[0], 0)),
            ]
            + [column(k) for k in range(count)],
            out_specs=pl.BlockSpec((part, HD), lambda h, *_: (0, h)),
        ),
        out_shape=jax.ShapeDtypeStruct((part, width), jnp.bfloat16),
        compiler_params=pltpu.CompilerParams(dimension_semantics=("arbitrary",)),
        name="vertical",
    )(slots, ok, quarter, queries, acc, stat, *([gathered] * count))


def tables(vertical, slash, slab_index, slab_blocks):
    heads, count = vertical.shape
    blocks = jnp.arange(lax.axis_size(SEQ) * slab_blocks, dtype=jnp.int32)
    flat = vertical.reshape(-1)
    used = jnp.any(flat[:, None] == blocks[None, :], axis=0)
    earlier = (blocks[None, :] // slab_blocks == flat[:, None] // slab_blocks) & (blocks[None, :] < flat[:, None])
    rank = jnp.sum((earlier & used[None, :]).astype(jnp.int32), axis=1)
    slots = flat // slab_blocks * CAP + rank
    mine = slab_index * slab_blocks + jnp.arange(slab_blocks, dtype=jnp.int32)
    gap = mine[None, :, None] - vertical[:, None, :]
    covered = jnp.any(gap[..., None] == slash[:, None, None, :], axis=3)
    ok = (gap > 0) & jnp.logical_not(covered)
    return slots, ok.astype(jnp.int32).reshape(-1)


def shards(queries, keys, values, vertical, slash):
    slab_blocks = queries.shape[0] // BLK
    slabs = lax.axis_size(SEQ)
    parts = lax.axis_size("head")
    slab_index = lax.axis_index(SEQ).astype(jnp.int32)
    base = (slab_index * slab_blocks).reshape(1)
    kv, packed = prep(vertical.reshape(-1), base, keys, values)
    gathered = lax.all_gather(packed, "y", axis=0, tiled=True)
    gathered = lax.all_gather(gathered, ("x", "z"), axis=0, tiled=True)

    def earlier(array, by):
        return lax.ppermute(array, SEQ, [(i, (i + by) % slabs) for i in range(slabs)])

    far_blocks = REACH % slab_blocks
    far = earlier(kv[slab_blocks - far_blocks :], 4)
    third, second, first = (earlier(kv, by) for by in (3, 2, 1))
    slots, ok = tables(vertical, slash, slab_index, slab_blocks)
    acc, stat = near(slash.reshape(-1), base, queries, far, third, second, first, kv)
    here = lax.axis_index("head").astype(jnp.int32)
    out = None
    for step in (1, 2, 3, 0):
        quarter = here ^ step
        piece = vertical_part(slots, ok, quarter.reshape(1), queries, acc, stat, gathered, parts)
        if step:
            piece = lax.ppermute(piece, "head", [(i, i ^ step) for i in range(parts)])
        if out is None:
            out = jnp.zeros((piece.shape[0], piece.shape[1] * parts), piece.dtype)
        out = lax.dynamic_update_slice_in_dim(out, piece, quarter * piece.shape[1], 1)
    return out


def solution(mesh):
    split = Mesh(mesh.devices.reshape(mesh.shape["head"], 4, 4, 2), ("head",) + SEQ)
    return jax.shard_map(
        shards,
        mesh=split,
        in_specs=(P(SEQ, "head"), P(SEQ, "head"), P(SEQ, "head"), P("head", None), P("head", None)),
        out_specs=P(SEQ + ("head",), None),
        check_vma=False,
    )
```

```python
import functools
import math

import jax
import jax.numpy as jnp
from jax import lax
from jax.experimental import pallas as pl
from jax.experimental.pallas import tpu as pltpu
from jax.sharding import Mesh
from jax.sharding import PartitionSpec as P

BLK = 128
HD = 128
REACH = 28
CAP = 4
NEG = -1e30
SEQ = ("x", "z", "y")
SCALE2 = math.log2(math.e) / math.sqrt(HD)


def prep_kernel(flat_ref, base_ref, keys_ref, values_ref, kv_ref, packed_ref):
    slab_blocks = kv_ref.shape[0]
    base = base_ref[0]

    def mark(entry, bits):
        local = flat_ref[entry] - base
        inside = (local >= 0) & (local < slab_blocks)
        return bits | jnp.where(inside, 1 << jnp.where(inside, local, 0), 0)

    bits = lax.fori_loop(0, flat_ref.shape[0], mark, jnp.int32(0))
    packed_ref[...] = jnp.zeros(packed_ref.shape, packed_ref.dtype)
    rank = jnp.int32(0)
    for block in range(slab_blocks):
        rows = pl.ds(block * BLK, BLK)
        kv_ref[block, :BLK, :] = keys_ref[rows, :].T
        kv_ref[block, BLK:, :] = values_ref[rows, :]
        used = (bits >> block) & 1

        @pl.when((used == 1) & (rank < CAP))
        def _(block=block, rank=rank):
            packed_ref[rank] = kv_ref[block]

        rank = rank + used


def prep(flat, base, keys, values):
    slab_blocks = keys.shape[0] // BLK
    whole = lambda shape: pl.BlockSpec(shape, lambda *_: (0,) * len(shape))
    return pl.pallas_call(
        prep_kernel,
        grid_spec=pltpu.PrefetchScalarGridSpec(
            num_scalar_prefetch=2,
            grid=(1,),
            in_specs=[whole(keys.shape), whole(values.shape)],
            out_specs=[whole((slab_blocks, 2 * BLK, HD)), whole((CAP, 2 * BLK, HD))],
        ),
        out_shape=[
            jax.ShapeDtypeStruct((slab_blocks, 2 * BLK, HD), jnp.bfloat16),
            jax.ShapeDtypeStruct((CAP, 2 * BLK, HD), jnp.bfloat16),
        ],
        name="prep",
    )(flat, base, keys, values)


def bias_columns(flags, rows):
    lanes = lax.broadcasted_iota(jnp.int32, (8, HD), 1)
    columns = jnp.zeros((8, HD), jnp.float32)
    for n, flag in enumerate(flags):
        columns = jnp.where(lanes == n, jnp.where(flag, 0.0, NEG).astype(jnp.float32), columns)
    return jnp.broadcast_to(columns[:1], (rows, HD)).astype(jnp.bfloat16)


def marker_rows(n):
    return (lax.broadcasted_iota(jnp.int32, (HD, BLK), 0) == n).astype(jnp.bfloat16)


def score_stage(q, flags, kts, score_ref, top_ref, causal=None, floor=None):
    left = jnp.concatenate([q, bias_columns(flags, q.shape[0])], axis=1)
    right = jnp.concatenate(
        [jnp.concatenate([kt, marker_rows(n)], axis=0) for n, kt in enumerate(kts)], axis=1
    )
    scores = jnp.dot(left, right, preferred_element_type=jnp.float32)
    parts = [scores[:, n * BLK : (n + 1) * BLK] for n in range(len(kts))]
    if causal is not None:
        parts[0] = jnp.where(causal, parts[0], NEG)
    for n, part in enumerate(parts):
        score_ref[:, n * BLK : (n + 1) * BLK] = part
    top = jnp.max(functools.reduce(jnp.maximum, parts), axis=1, keepdims=True) * SCALE2
    if floor is not None:
        top = jnp.maximum(top, floor)
    top_ref[...] = jnp.broadcast_to(top, top_ref.shape)


def weight_stage(score_ref, top_ref, vs):
    top = top_ref[...]
    rounded = []
    for n in range(len(vs)):
        weights = jnp.exp2(score_ref[:, n * BLK : (n + 1) * BLK] * SCALE2 - top)
        rounded.append(weights.astype(jnp.bfloat16))
    v = jnp.concatenate(vs, axis=0)
    v = jnp.concatenate([v, jnp.ones(v.shape, v.dtype)], axis=1)
    return jnp.dot(jnp.concatenate(rounded, axis=1), v, preferred_element_type=jnp.float32)


def near_kernel(
    slash_ref, base_ref, q_ref, far_ref, third_ref, second_ref, first_ref, own_ref, acc_ref, stat_ref, band, score_a, score_b, top_a, top_b, sems
):
    head = pl.program_id(0)
    slab_blocks = own_ref.shape[0]
    slash_count = slash_ref.shape[0] // pl.num_programs(0)

    @pl.when(head == 0)
    def _():
        start = 0
        copies = []
        for number, part in enumerate((far_ref, third_ref, second_ref, first_ref, own_ref)):
            copies.append(pltpu.make_async_copy(part, band.at[pl.ds(start, part.shape[0])], sems.at[number]))
            start += part.shape[0]
        for copy in copies:
            copy.start()
        for copy in copies:
            copy.wait()

    lanes = lax.broadcasted_iota(jnp.int32, (BLK, HD), 1)
    causal = lax.broadcasted_iota(jnp.int32, (BLK, BLK), 0) >= lanes
    base = base_ref[0]
    offsets = [slash_ref[head * slash_count + n] for n in range(slash_count)]
    buffers = ((score_a, top_a), (score_b, top_b))

    def places(index):
        return [index + REACH] + [index + REACH - s for s in offsets]

    def begin(index):
        flags = [True] + [base + index - s >= 0 for s in offsets]
        kts = [band[p, :BLK, :] for p in places(index)]
        score_stage(q_ref[index * BLK : (index + 1) * BLK, :], flags, kts, *buffers[index % 2], causal=causal)

    def finish(index):
        rows = slice(index * BLK, (index + 1) * BLK)
        score_ref, top_ref = buffers[index % 2]
        mixed = weight_stage(score_ref, top_ref, [band[p, BLK:, :] for p in places(index)])
        acc_ref[rows, :] = mixed[:, :HD]
        stat = jnp.where(lanes == 2 * head, top_ref[...], stat_ref[rows, :])
        stat_ref[rows, :] = jnp.where(lanes == 2 * head + 1, mixed[:, HD:], stat)

    begin(0)
    for index in range(slab_blocks):
        if index + 1 < slab_blocks:
            begin(index + 1)
        finish(index)


def near(slash, base, queries, far, third, second, first, own):
    rows, width = queries.shape
    heads = width // HD
    slab_blocks = rows // BLK
    slash_count = slash.shape[0] // heads
    hbm = pl.BlockSpec(memory_space=pl.ANY)
    return pl.pallas_call(
        near_kernel,
        grid_spec=pltpu.PrefetchScalarGridSpec(
            num_scalar_prefetch=2,
            grid=(heads,),
            in_specs=[pl.BlockSpec((rows, HD), lambda h, *_: (0, h))] + [hbm] * 5,
            out_specs=[
                pl.BlockSpec((rows, HD), lambda h, *_: (0, h)),
                pl.BlockSpec((rows, HD), lambda h, *_: (0, 0)),
            ],
            scratch_shapes=[
                pltpu.VMEM((REACH + slab_blocks, 2 * BLK, HD), jnp.bfloat16),
                pltpu.VMEM((BLK, (slash_count + 1) * BLK), jnp.float32),
                pltpu.VMEM((BLK, (slash_count + 1) * BLK), jnp.float32),
                pltpu.VMEM((BLK, HD), jnp.float32),
                pltpu.VMEM((BLK, HD), jnp.float32),
                pltpu.SemaphoreType.DMA((5,)),
            ],
        ),
        out_shape=[
            jax.ShapeDtypeStruct((rows, width), jnp.float32),
            jax.ShapeDtypeStruct((rows, HD), jnp.float32),
        ],
        compiler_params=pltpu.CompilerParams(dimension_semantics=("arbitrary",)),
        name="near",
    )(slash, base, queries, far, third, second, first, own)


def vertical_kernel(slab_blocks, count, slot_ref, ok_ref, quarters_ref, *refs):
    ins, refs = refs[:6], refs[6:]
    columns, refs = refs[:count], refs[count:]
    outs, (score_a, score_b, top_a, top_b) = refs[:2], refs[2:]
    head = pl.program_id(0)
    blocks = outs[0].shape[0] // BLK
    lanes = lax.broadcasted_iota(jnp.int32, (BLK, HD), 1)
    kts = [c[0, :BLK, :] for c in columns]
    vs = [c[0, BLK:, :] for c in columns]
    buffers = ((score_a, top_a), (score_b, top_b))
    work = [(part, block) for part in range(2) for block in range(blocks)]

    def near_stat(part, block, which):
        stat = ins[3 * part + 2][block * BLK : (block + 1) * BLK, :]
        return jnp.sum(jnp.where(lanes == 2 * head + which, stat, 0.0), axis=1, keepdims=True)

    def begin(number):
        part, block = work[number]
        first = (head * slab_blocks + quarters_ref[part] * blocks + block) * count
        flags = [ok_ref[first + k] > 0 for k in range(count)]
        q = ins[3 * part][block * BLK : (block + 1) * BLK, :]
        score_stage(q, flags, kts, *buffers[number % 2], floor=near_stat(part, block, 0))

    def finish(number):
        part, block = work[number]
        rows = slice(block * BLK, (block + 1) * BLK)
        score_ref, top_ref = buffers[number % 2]
        mixed = weight_stage(score_ref, top_ref, vs)
        shrink = jnp.exp2(near_stat(part, block, 0) - top_ref[...])
        total = mixed[:, HD:] + near_stat(part, block, 1) * shrink
        whole = mixed[:, :HD] + ins[3 * part + 1][rows, :] * shrink
        outs[part][rows, :] = (whole / total).astype(outs[part].dtype)

    begin(0)
    for number in range(len(work)):
        if number + 1 < len(work):
            begin(number + 1)
        finish(number)


def vertical_half(slots, ok, quarters, queries, acc, stat, gathered, parts):
    rows, width = queries.shape
    heads = width // HD
    count = slots.shape[0] // heads
    part = rows // parts

    def column(k):
        return pl.BlockSpec((1, 2 * BLK, HD), lambda h, slot, ok, quarters: (slot[h * count + k], 0, 0))

    def own(which, fixed=False):
        return pl.BlockSpec((part, HD), lambda h, slot, ok, quarters: (quarters[which], 0 if fixed else h))

    return pl.pallas_call(
        functools.partial(vertical_kernel, rows // BLK, count),
        grid_spec=pltpu.PrefetchScalarGridSpec(
            num_scalar_prefetch=3,
            grid=(heads,),
            in_specs=[own(0), own(0), own(0, True), own(1), own(1), own(1, True)] + [column(k) for k in range(count)],
            out_specs=[pl.BlockSpec((part, HD), lambda h, *_: (0, h))] * 2,
            scratch_shapes=[
                pltpu.VMEM((BLK, count * BLK), jnp.float32),
                pltpu.VMEM((BLK, count * BLK), jnp.float32),
                pltpu.VMEM((BLK, HD), jnp.float32),
                pltpu.VMEM((BLK, HD), jnp.float32),
            ],
        ),
        out_shape=[jax.ShapeDtypeStruct((part, width), jnp.bfloat16)] * 2,
        compiler_params=pltpu.CompilerParams(dimension_semantics=("arbitrary",)),
        name="vertical",
    )(slots, ok, quarters, *([queries, acc, stat] * 2), *([gathered] * count))


def tables(vertical, slash, slab_index, slab_blocks):
    heads, count = vertical.shape
    blocks = jnp.arange(lax.axis_size(SEQ) * slab_blocks, dtype=jnp.int32)
    flat = vertical.reshape(-1)
    used = jnp.any(flat[:, None] == blocks[None, :], axis=0)
    earlier = (blocks[None, :] // slab_blocks == flat[:, None] // slab_blocks) & (blocks[None, :] < flat[:, None])
    rank = jnp.sum((earlier & used[None, :]).astype(jnp.int32), axis=1)
    slots = flat // slab_blocks * CAP + rank
    mine = slab_index * slab_blocks + jnp.arange(slab_blocks, dtype=jnp.int32)
    gap = mine[None, :, None] - vertical[:, None, :]
    covered = jnp.any(gap[..., None] == slash[:, None, None, :], axis=3)
    ok = (gap > 0) & jnp.logical_not(covered)
    return slots, ok.astype(jnp.int32).reshape(-1)


def shards(queries, keys, values, vertical, slash):
    slab_blocks = queries.shape[0] // BLK
    slabs = lax.axis_size(SEQ)
    parts = lax.axis_size("head")
    slab_index = lax.axis_index(SEQ).astype(jnp.int32)
    base = (slab_index * slab_blocks).reshape(1)
    kv, packed = prep(vertical.reshape(-1), base, keys, values)
    gathered = lax.all_gather(packed, "y", axis=0, tiled=True)
    gathered = lax.all_gather(gathered, ("x", "z"), axis=0, tiled=True)

    def earlier(array, by):
        return lax.ppermute(array, SEQ, [(i, (i + by) % slabs) for i in range(slabs)])

    far_blocks = REACH % slab_blocks
    far = earlier(kv[slab_blocks - far_blocks :], 4)
    third, second, first = (earlier(kv, by) for by in (3, 2, 1))
    slots, ok = tables(vertical, slash, slab_index, slab_blocks)
    acc, stat = near(slash.reshape(-1), base, queries, far, third, second, first, kv)
    here = lax.axis_index("head").astype(jnp.int32)
    steps = ((2, 3), (1, 0))
    pieces = {}
    for pair in steps:
        quarters = jnp.stack([here ^ step for step in pair])
        done = vertical_half(slots, ok, quarters, queries, acc, stat, gathered, parts)
        for step, piece in zip(pair, done):
            pieces[step] = lax.ppermute(piece, "head", [(i, i ^ step) for i in range(parts)]) if step else piece
    width = queries.shape[1]
    out = jnp.zeros((pieces[0].shape[0], width * parts), pieces[0].dtype)
    for step in (0, 1, 2, 3):
        out = lax.dynamic_update_slice_in_dim(out, pieces[step], (here ^ step) * width, 1)
    return out


def solution(mesh):
    split = Mesh(mesh.devices.reshape(mesh.shape["head"], 4, 4, 2), ("head",) + SEQ)
    return jax.shard_map(
        shards,
        mesh=split,
        in_specs=(P(SEQ, "head"), P(SEQ, "head"), P(SEQ, "head"), P("head", None), P("head", None)),
        out_specs=P(SEQ + ("head",), None),
        check_vma=False,
    )
```

```python
import functools
import math

import jax
import jax.numpy as jnp
from jax import lax
from jax.experimental import pallas as pl
from jax.experimental.pallas import tpu as pltpu
from jax.sharding import Mesh
from jax.sharding import PartitionSpec as P

BLK = 128
HD = 128
REACH = 28
CAP = 4
NEG = -1e30
SEQ = ("x", "z", "y")
SCALE2 = math.log2(math.e) / math.sqrt(HD)


def cost(row_blocks, moved):
    return pl.CostEstimate(flops=row_blocks * 4 * BLK * HD, bytes_accessed=moved, transcendentals=row_blocks * BLK)


def prep_kernel(flat_ref, base_ref, keys_ref, values_ref, kv_ref, packed_ref):
    slab_blocks = kv_ref.shape[0]
    base = base_ref[0]

    def mark(entry, bits):
        local = flat_ref[entry] - base
        inside = (local >= 0) & (local < slab_blocks)
        return bits | jnp.where(inside, 1 << jnp.where(inside, local, 0), 0)

    bits = lax.fori_loop(0, flat_ref.shape[0], mark, jnp.int32(0))
    packed_ref[...] = jnp.zeros(packed_ref.shape, packed_ref.dtype)
    rank = jnp.int32(0)
    for block in range(slab_blocks):
        rows = pl.ds(block * BLK, BLK)
        kv_ref[block, :BLK, :] = keys_ref[rows, :].T
        kv_ref[block, BLK:, :] = values_ref[rows, :]
        used = (bits >> block) & 1

        @pl.when((used == 1) & (rank < CAP))
        def _(block=block, rank=rank):
            packed_ref[rank] = kv_ref[block]

        rank = rank + used


def prep(flat, base, keys, values):
    slab_blocks = keys.shape[0] // BLK
    whole = lambda shape: pl.BlockSpec(shape, lambda *_: (0,) * len(shape))
    return pl.pallas_call(
        prep_kernel,
        grid_spec=pltpu.PrefetchScalarGridSpec(
            num_scalar_prefetch=2,
            grid=(1,),
            in_specs=[whole(keys.shape), whole(values.shape)],
            out_specs=[whole((slab_blocks, 2 * BLK, HD)), whole((CAP, 2 * BLK, HD))],
        ),
        out_shape=[
            jax.ShapeDtypeStruct((slab_blocks, 2 * BLK, HD), jnp.bfloat16),
            jax.ShapeDtypeStruct((CAP, 2 * BLK, HD), jnp.bfloat16),
        ],
        name="prep",
    )(flat, base, keys, values)


def bias_columns(flags, rows):
    lanes = lax.broadcasted_iota(jnp.int32, (8, HD), 1)
    columns = jnp.zeros((8, HD), jnp.float32)
    for n, flag in enumerate(flags):
        columns = jnp.where(lanes == n, jnp.where(flag, 0.0, NEG).astype(jnp.float32), columns)
    return jnp.broadcast_to(columns[:1], (rows, HD)).astype(jnp.bfloat16)


def marker_rows(n):
    return (lax.broadcasted_iota(jnp.int32, (HD, BLK), 0) == n).astype(jnp.bfloat16)


def score_stage(q, flags, kts, score_ref, top_ref, causal=None, floor=None):
    left = jnp.concatenate([q, bias_columns(flags, q.shape[0])], axis=1)
    right = jnp.concatenate(
        [jnp.concatenate([kt, marker_rows(n)], axis=0) for n, kt in enumerate(kts)], axis=1
    )
    scores = jnp.dot(left, right, preferred_element_type=jnp.float32)
    parts = [scores[:, n * BLK : (n + 1) * BLK] * SCALE2 for n in range(len(kts))]
    if causal is not None:
        parts[0] = jnp.where(causal, parts[0], NEG)
    for n, part in enumerate(parts):
        score_ref[:, n * BLK : (n + 1) * BLK] = part
    top = jnp.max(functools.reduce(jnp.maximum, parts), axis=1, keepdims=True)
    if floor is not None:
        top = jnp.maximum(top, floor)
    top_ref[...] = jnp.broadcast_to(top, top_ref.shape)


def weight_stage(score_ref, top_ref, vs):
    top = top_ref[...]
    rounded = []
    for n in range(len(vs)):
        weights = jnp.exp2(score_ref[:, n * BLK : (n + 1) * BLK] - top)
        rounded.append(weights.astype(jnp.bfloat16))
    v = jnp.concatenate(vs, axis=0)
    v = jnp.concatenate([v, jnp.ones(v.shape, v.dtype)], axis=1)
    return jnp.dot(jnp.concatenate(rounded, axis=1), v, preferred_element_type=jnp.float32)


def near_kernel(
    slash_ref, base_ref, q_ref, far_ref, third_ref, second_ref, first_ref, own_ref, acc_ref, stat_ref, band, score_a, score_b, top_a, top_b, sems
):
    head = pl.program_id(0)
    slab_blocks = own_ref.shape[0]
    slash_count = slash_ref.shape[0] // pl.num_programs(0)

    @pl.when(head == 0)
    def _():
        start = 0
        copies = []
        for number, part in enumerate((far_ref, third_ref, second_ref, first_ref, own_ref)):
            copies.append(pltpu.make_async_copy(part, band.at[pl.ds(start, part.shape[0])], sems.at[number]))
            start += part.shape[0]
        for copy in copies:
            copy.start()
        for copy in copies:
            copy.wait()

    lanes = lax.broadcasted_iota(jnp.int32, (BLK, HD), 1)
    causal = lax.broadcasted_iota(jnp.int32, (BLK, BLK), 0) >= lanes
    base = base_ref[0]
    offsets = [slash_ref[head * slash_count + n] for n in range(slash_count)]
    buffers = ((score_a, top_a), (score_b, top_b))

    def places(index):
        return [index + REACH] + [index + REACH - s for s in offsets]

    def begin(index):
        flags = [True] + [base + index - s >= 0 for s in offsets]
        kts = [band[p, :BLK, :] for p in places(index)]
        score_stage(q_ref[index * BLK : (index + 1) * BLK, :], flags, kts, *buffers[index % 2], causal=causal)

    def finish(index):
        rows = slice(index * BLK, (index + 1) * BLK)
        score_ref, top_ref = buffers[index % 2]
        mixed = weight_stage(score_ref, top_ref, [band[p, BLK:, :] for p in places(index)])
        acc_ref[rows, :] = mixed[:, :HD]
        stat = jnp.where(lanes == 2 * head, top_ref[...], stat_ref[rows, :])
        stat_ref[rows, :] = jnp.where(lanes == 2 * head + 1, mixed[:, HD:], stat)

    begin(0)
    for index in range(slab_blocks):
        if index + 1 < slab_blocks:
            begin(index + 1)
        finish(index)


def near(slash, base, queries, far, third, second, first, own):
    rows, width = queries.shape
    heads = width // HD
    slab_blocks = rows // BLK
    slash_count = slash.shape[0] // heads
    hbm = pl.BlockSpec(memory_space=pl.ANY)
    return pl.pallas_call(
        near_kernel,
        grid_spec=pltpu.PrefetchScalarGridSpec(
            num_scalar_prefetch=2,
            grid=(heads,),
            in_specs=[pl.BlockSpec((rows, HD), lambda h, *_: (0, h))] + [hbm] * 5,
            out_specs=[
                pl.BlockSpec((rows, HD), lambda h, *_: (0, h)),
                pl.BlockSpec((rows, HD), lambda h, *_: (0, 0)),
            ],
            scratch_shapes=[
                pltpu.VMEM((REACH + slab_blocks, 2 * BLK, HD), jnp.bfloat16),
                pltpu.VMEM((BLK, (slash_count + 1) * BLK), jnp.float32),
                pltpu.VMEM((BLK, (slash_count + 1) * BLK), jnp.float32),
                pltpu.VMEM((BLK, HD), jnp.float32),
                pltpu.VMEM((BLK, HD), jnp.float32),
                pltpu.SemaphoreType.DMA((5,)),
            ],
        ),
        out_shape=[
            jax.ShapeDtypeStruct((rows, width), jnp.float32),
            jax.ShapeDtypeStruct((rows, HD), jnp.float32),
        ],
        compiler_params=pltpu.CompilerParams(dimension_semantics=("arbitrary",)),
        cost_estimate=cost(rows * heads * (slash_count + 1), rows * width * 8),
        name="near",
    )(slash, base, queries, far, third, second, first, own)


def vertical_kernel(slab_blocks, count, slot_ref, ok_ref, quarters_ref, *refs):
    ins, refs = refs[:6], refs[6:]
    columns, refs = refs[:count], refs[count:]
    outs, (score_a, score_b, top_a, top_b) = refs[:2], refs[2:]
    head = pl.program_id(0)
    blocks = outs[0].shape[0] // BLK
    lanes = lax.broadcasted_iota(jnp.int32, (BLK, HD), 1)
    kts = [c[0, :BLK, :] for c in columns]
    vs = [c[0, BLK:, :] for c in columns]
    buffers = ((score_a, top_a), (score_b, top_b))
    work = [(part, block) for part in range(2) for block in range(blocks)]

    def near_stat(part, block, which):
        stat = ins[3 * part + 2][block * BLK : (block + 1) * BLK, :]
        return jnp.sum(jnp.where(lanes == 2 * head + which, stat, 0.0), axis=1, keepdims=True)

    def begin(number):
        part, block = work[number]
        first = (head * slab_blocks + quarters_ref[part] * blocks + block) * count
        flags = [ok_ref[first + k] > 0 for k in range(count)]
        q = ins[3 * part][block * BLK : (block + 1) * BLK, :]
        score_stage(q, flags, kts, *buffers[number % 2], floor=near_stat(part, block, 0))

    def finish(number):
        part, block = work[number]
        rows = slice(block * BLK, (block + 1) * BLK)
        score_ref, top_ref = buffers[number % 2]
        mixed = weight_stage(score_ref, top_ref, vs)
        shrink = jnp.exp2(near_stat(part, block, 0) - top_ref[...])
        total = mixed[:, HD:] + near_stat(part, block, 1) * shrink
        whole = mixed[:, :HD] + ins[3 * part + 1][rows, :] * shrink
        outs[part][rows, :] = (whole / total).astype(outs[part].dtype)

    begin(0)
    for number in range(len(work)):
        if number + 1 < len(work):
            begin(number + 1)
        finish(number)


def vertical_half(slots, ok, quarters, queries, acc, stat, gathered, parts):
    rows, width = queries.shape
    heads = width // HD
    count = slots.shape[0] // heads
    part = rows // parts

    def column(k):
        return pl.BlockSpec((1, 2 * BLK, HD), lambda h, slot, ok, quarters: (slot[h * count + k], 0, 0))

    def own(which, fixed=False):
        return pl.BlockSpec((part, HD), lambda h, slot, ok, quarters: (quarters[which], 0 if fixed else h))

    return pl.pallas_call(
        functools.partial(vertical_kernel, rows // BLK, count),
        grid_spec=pltpu.PrefetchScalarGridSpec(
            num_scalar_prefetch=3,
            grid=(heads,),
            in_specs=[own(0), own(0), own(0, True), own(1), own(1), own(1, True)] + [column(k) for k in range(count)],
            out_specs=[pl.BlockSpec((part, HD), lambda h, *_: (0, h))] * 2,
            scratch_shapes=[
                pltpu.VMEM((BLK, count * BLK), jnp.float32),
                pltpu.VMEM((BLK, count * BLK), jnp.float32),
                pltpu.VMEM((BLK, HD), jnp.float32),
                pltpu.VMEM((BLK, HD), jnp.float32),
            ],
        ),
        out_shape=[jax.ShapeDtypeStruct((part, width), jnp.bfloat16)] * 2,
        compiler_params=pltpu.CompilerParams(dimension_semantics=("arbitrary",)),
        cost_estimate=cost(2 * part * heads * count, part * width * 32),
        name="vertical",
    )(slots, ok, quarters, *([queries, acc, stat] * 2), *([gathered] * count))


def tables(vertical, slash, slab_index, slab_blocks, row):
    blocks = jnp.arange(lax.axis_size(SEQ) * slab_blocks, dtype=jnp.int32)
    flat = vertical.reshape(-1)
    used = jnp.any(flat[:, None] == blocks[None, :], axis=0)
    earlier = (blocks[None, :] // slab_blocks == flat[:, None] // slab_blocks) & (blocks[None, :] < flat[:, None])
    rank = jnp.sum((earlier & used[None, :]).astype(jnp.int32), axis=1)
    slots = (flat // slab_blocks ^ row) * CAP + rank
    mine = slab_index * slab_blocks + jnp.arange(slab_blocks, dtype=jnp.int32)
    gap = mine[None, :, None] - vertical[:, None, :]
    covered = jnp.any(gap[..., None] == slash[:, None, None, :], axis=3)
    ok = (gap > 0) & jnp.logical_not(covered)
    return slots, ok.astype(jnp.int32).reshape(-1)


def shards(queries, keys, values, vertical, slash):
    slab_blocks = queries.shape[0] // BLK
    parts = lax.axis_size("head")
    slab_index = lax.axis_index(SEQ).astype(jnp.int32)
    base = (slab_index * slab_blocks).reshape(1)
    kv, packed = prep(vertical.reshape(-1), base, keys, values)
    slabs = lax.axis_size(SEQ)
    pair = lax.axis_size("y")

    def swapped(array):
        return lax.ppermute(array, "y", [(i, pair - 1 - i) for i in range(pair)])

    def from_before(array):
        return lax.ppermute(array, SEQ, [(i, (i + pair) % slabs) for i in range(slabs)])

    gathered = lax.all_gather(jnp.stack([packed, swapped(packed)]), ("x", "z"), axis=0, tiled=True)
    gathered = gathered.reshape(-1, *packed.shape[1:])
    upper = lax.axis_index("y") == 1
    second = from_before(kv)
    fourth = from_before(second)
    first = swapped(jnp.where(upper, second, kv))
    third = swapped(jnp.where(upper, fourth, second))
    far = fourth[slab_blocks - REACH % slab_blocks :]
    slots, ok = tables(vertical, slash, slab_index, slab_blocks, lax.axis_index("y").astype(jnp.int32))
    acc, stat = near(slash.reshape(-1), base, queries, far, third, second, first, kv)
    here = lax.axis_index("head").astype(jnp.int32)

    def half(pair):
        quarters = jnp.stack([here ^ step for step in pair])
        return vertical_half(slots, ok, quarters, queries, acc, stat, gathered, parts)

    def sent(piece, step):
        return lax.ppermute(piece, "head", [(i, i ^ step) for i in range(parts)])

    second_piece, third_piece = half((2, 3))
    first_piece, own_piece = half((1, 0))
    pieces = [own_piece, sent(first_piece, 1), sent(second_piece, 2), sent(third_piece, 3)]
    width = queries.shape[1]
    out = jnp.zeros((pieces[0].shape[0], width * parts), pieces[0].dtype)
    for step in (0, 1, 2, 3):
        out = lax.dynamic_update_slice_in_dim(out, pieces[step], (here ^ step) * width, 1)
    return out


def solution(mesh):
    split = Mesh(mesh.devices.reshape(mesh.shape["head"], 4, 4, 2), ("head",) + SEQ)
    return jax.shard_map(
        shards,
        mesh=split,
        in_specs=(P(SEQ, "head"), P(SEQ, "head"), P(SEQ, "head"), P("head", None), P("head", None)),
        out_specs=P(SEQ + ("head",), None),
        check_vma=False,
    )
```

```python
import functools
import math

import jax
import jax.numpy as jnp
from jax import lax
from jax.experimental import pallas as pl
from jax.experimental.pallas import tpu as pltpu
from jax.sharding import Mesh
from jax.sharding import PartitionSpec as P

BLK = 128
HD = 128
REACH = 28
CAP = 4
NEG = -1e30
SEQ = ("x", "z", "y")
SCALE2 = math.log2(math.e) / math.sqrt(HD)


def cost(row_blocks, moved):
    return pl.CostEstimate(flops=row_blocks * 4 * BLK * HD, bytes_accessed=moved, transcendentals=row_blocks * BLK)


def prep_kernel(vertical_ref, base_ref, keys_ref, values_ref, kv_ref, packed_ref):
    slab_blocks = kv_ref.shape[0]
    base = base_ref[0]

    bits = jnp.int32(0)
    for head in range(vertical_ref.shape[0]):
        for number in range(vertical_ref.shape[1]):
            local = vertical_ref[head, number] - base
            inside = (local >= 0) & (local < slab_blocks)
            bits = bits | jnp.where(inside, 1 << jnp.where(inside, local, 0), 0)
    packed_ref[...] = jnp.zeros(packed_ref.shape, packed_ref.dtype)
    rank = jnp.int32(0)
    for block in range(slab_blocks):
        rows = pl.ds(block * BLK, BLK)
        kv_ref[block, :BLK, :] = keys_ref[rows, :].T
        kv_ref[block, BLK:, :] = values_ref[rows, :]
        used = (bits >> block) & 1

        @pl.when((used == 1) & (rank < CAP))
        def _(block=block, rank=rank):
            packed_ref[rank] = kv_ref[block]

        rank = rank + used


def prep(vertical, base, keys, values):
    slab_blocks = keys.shape[0] // BLK
    whole = lambda shape: pl.BlockSpec(shape, lambda *_: (0,) * len(shape))
    return pl.pallas_call(
        prep_kernel,
        grid_spec=pltpu.PrefetchScalarGridSpec(
            num_scalar_prefetch=2,
            grid=(1,),
            in_specs=[whole(keys.shape), whole(values.shape)],
            out_specs=[whole((slab_blocks, 2 * BLK, HD)), whole((CAP, 2 * BLK, HD))],
        ),
        out_shape=[
            jax.ShapeDtypeStruct((slab_blocks, 2 * BLK, HD), jnp.bfloat16),
            jax.ShapeDtypeStruct((CAP, 2 * BLK, HD), jnp.bfloat16),
        ],
        name="prep",
    )(vertical, base, keys, values)


def bias_columns(flags, rows):
    lanes = lax.broadcasted_iota(jnp.int32, (8, HD), 1)
    columns = jnp.zeros((8, HD), jnp.float32)
    for n, flag in enumerate(flags):
        columns = jnp.where(lanes == n, jnp.where(flag, 0.0, NEG).astype(jnp.float32), columns)
    return jnp.broadcast_to(columns[:1], (rows, HD)).astype(jnp.bfloat16)


def marker_rows(n):
    return (lax.broadcasted_iota(jnp.int32, (HD, BLK), 0) == n).astype(jnp.bfloat16)


def score_stage(q, flags, kts, score_ref, top_ref, causal=None, floor=None):
    left = jnp.concatenate([q, bias_columns(flags, q.shape[0])], axis=1)
    right = jnp.concatenate(
        [jnp.concatenate([kt, marker_rows(n)], axis=0) for n, kt in enumerate(kts)], axis=1
    )
    scores = jnp.dot(left, right, preferred_element_type=jnp.float32)
    parts = [scores[:, n * BLK : (n + 1) * BLK] * SCALE2 for n in range(len(kts))]
    if causal is not None:
        parts[0] = jnp.where(causal, parts[0], NEG)
    for n, part in enumerate(parts):
        score_ref[:, n * BLK : (n + 1) * BLK] = part
    top = jnp.max(functools.reduce(jnp.maximum, parts), axis=1, keepdims=True)
    if floor is not None:
        top = jnp.maximum(top, floor)
    top_ref[...] = jnp.broadcast_to(top, top_ref.shape)


def weight_stage(score_ref, top_ref, vs):
    top = top_ref[...]
    rounded = []
    for n in range(len(vs)):
        weights = jnp.exp2(score_ref[:, n * BLK : (n + 1) * BLK] - top)
        rounded.append(weights.astype(jnp.bfloat16))
    v = jnp.concatenate(vs, axis=0)
    v = jnp.concatenate([v, jnp.ones(v.shape, v.dtype)], axis=1)
    return jnp.dot(jnp.concatenate(rounded, axis=1), v, preferred_element_type=jnp.float32)


def near_kernel(
    slash_ref, base_ref, q_ref, next_q_ref, far_ref, third_ref, second_ref, first_ref, own_ref, near_ref, stat_ref, band, score_a, score_b, top_a, top_b, sems
):
    head = pl.program_id(0)
    heads = pl.num_programs(0)
    slab_blocks = own_ref.shape[0]
    slash_count = slash_ref.shape[1]
    lanes = lax.broadcasted_iota(jnp.int32, (BLK, HD), 1)
    causal = lax.broadcasted_iota(jnp.int32, (BLK, BLK), 0) >= lanes
    base = base_ref[0]
    buffers = ((score_a, top_a), (score_b, top_b))

    def offsets_of(which):
        return [slash_ref[which, n] for n in range(slash_count)]

    def places(index, offsets):
        return [index + REACH] + [index + REACH - s for s in offsets]

    def begin(q, index, offsets):
        flags = [True] + [base + index - s >= 0 for s in offsets]
        kts = [band[p, :BLK, :] for p in places(index, offsets)]
        score_stage(q[index * BLK : (index + 1) * BLK, :], flags, kts, *buffers[index % 2], causal=causal)

    def finish(index, offsets):
        rows = slice(index * BLK, (index + 1) * BLK)
        score_ref, top_ref = buffers[index % 2]
        mixed = weight_stage(score_ref, top_ref, [band[p, BLK:, :] for p in places(index, offsets)])
        total = mixed[:, HD:]
        near_ref[rows, :] = mixed[:, :HD] / total
        stat_ref[rows, :] = jnp.where(lanes == head, top_ref[...] + jnp.log2(total), stat_ref[rows, :])

    offsets = offsets_of(head)
    following = offsets_of(jnp.minimum(head + 1, heads - 1))

    @pl.when(head == 0)
    def _():
        start = 0
        copies = []
        for number, part in enumerate((far_ref, third_ref, second_ref, first_ref, own_ref)):
            copies.append(pltpu.make_async_copy(part, band.at[pl.ds(start, part.shape[0])], sems.at[number]))
            start += part.shape[0]
        for copy in copies:
            copy.start()
        for copy in copies:
            copy.wait()
        begin(q_ref, 0, offsets)

    for index in range(slab_blocks):
        if index + 1 < slab_blocks:
            begin(q_ref, index + 1, offsets)
        else:
            begin(next_q_ref, 0, following)
        finish(index, offsets)


def near(slash, base, queries, far, third, second, first, own):
    rows, width = queries.shape
    heads = width // HD
    slab_blocks = rows // BLK
    slash_count = slash.shape[1]
    assert slab_blocks % 2 == 0
    hbm = pl.BlockSpec(memory_space=pl.ANY)
    return pl.pallas_call(
        near_kernel,
        grid_spec=pltpu.PrefetchScalarGridSpec(
            num_scalar_prefetch=2,
            grid=(heads,),
            in_specs=[
                pl.BlockSpec((rows, HD), lambda h, *_: (0, h)),
                pl.BlockSpec((BLK, HD), lambda h, *_: (0, jnp.minimum(h + 1, heads - 1))),
            ]
            + [hbm] * 5,
            out_specs=[
                pl.BlockSpec((rows, HD), lambda h, *_: (0, h)),
                pl.BlockSpec((rows, HD), lambda h, *_: (0, 0)),
            ],
            scratch_shapes=[
                pltpu.VMEM((REACH + slab_blocks, 2 * BLK, HD), jnp.bfloat16),
                pltpu.VMEM((BLK, (slash_count + 1) * BLK), jnp.float32),
                pltpu.VMEM((BLK, (slash_count + 1) * BLK), jnp.float32),
                pltpu.VMEM((BLK, HD), jnp.float32),
                pltpu.VMEM((BLK, HD), jnp.float32),
                pltpu.SemaphoreType.DMA((5,)),
            ],
        ),
        out_shape=[
            jax.ShapeDtypeStruct((rows, width), jnp.float32),
            jax.ShapeDtypeStruct((rows, HD), jnp.float32),
        ],
        compiler_params=pltpu.CompilerParams(dimension_semantics=("arbitrary",)),
        cost_estimate=cost(rows * heads * (slash_count + 1), rows * width * 8),
        name="near",
    )(slash, base, queries, queries, far, third, second, first, own)


def vertical_kernel(count, slot_ref, ok_ref, quarters_ref, *refs):
    ins, refs = refs[:8], refs[8:]
    colours, refs = (refs[:5], refs[5:10]), refs[10:]
    outs, (columns, score_a, score_b, top_a, top_b, stat_a, stat_b, sems) = refs[:2], refs[2:]
    step = pl.program_id(0)
    heads = 2 * pl.num_programs(0)
    depth = columns.shape[0]
    piece = colours[0][0].shape[0]
    part_rows = outs[0].shape[0]
    blocks = part_rows // BLK
    lanes = lax.broadcasted_iota(jnp.int32, (2 * part_rows, HD), 1)
    buffers = ((score_a, top_a, stat_a), (score_b, top_b, stat_b))

    def fetch(which):
        place = which % depth
        for k in range(count):
            slot = slot_ref[which * count + k]
            colour, region, inner = slot // (4 * piece), slot // piece % 4, slot % piece
            half = piece // 2
            for number, (own, ahead, low, high, behind) in enumerate(colours):

                @pl.when(colour == number)
                def _(own=own, ahead=ahead, low=low, high=high, behind=behind, k=k, region=region, inner=inner):
                    def take(condition, source, index):
                        @pl.when(condition)
                        def _():
                            pltpu.make_async_copy(source.at[index], columns.at[place, k], sems.at[place]).start()

                    take(region == 0, own, inner)
                    take(region == 1, ahead, inner)
                    take((region == 2) & (inner < half), low, inner)
                    take((region == 2) & (inner >= half), high, inner - half)
                    take(region == 3, behind, inner)

    def arrive(which):
        place = which % depth
        pltpu.make_async_copy(columns.at[place], columns.at[place], sems.at[place]).wait()

    def guarded(action, which):
        @pl.when(which < heads)
        def _():
            action(which)

    def begin(which, qs, buffer):
        score_ref, top_ref, stat_ref = buffer
        biases = []
        for part in range(2):
            for block in range(blocks):
                here = quarters_ref[part] * blocks + block
                flags = [ok_ref[which, here * count + k] > 0 for k in range(count)]
                biases.append(bias_columns(flags, BLK))
        left = jnp.concatenate([jnp.concatenate(qs, axis=0), jnp.concatenate(biases, axis=0)], axis=1)
        stat = jnp.concatenate([ins[3][...], ins[7][...]], axis=0)
        top = jnp.sum(jnp.where(lanes == which, stat, 0.0), axis=1, keepdims=True)
        stat_ref[...] = jnp.broadcast_to(top, stat_ref.shape)
        tops = []
        for k in range(0, count, 2):
            pair = [
                jnp.concatenate([columns[which % depth, n, :BLK], marker_rows(n)], axis=0) for n in (k, k + 1)
            ]
            scores = jnp.dot(left, jnp.concatenate(pair, axis=1), preferred_element_type=jnp.float32) * SCALE2
            score_ref[:, k * BLK : (k + 2) * BLK] = scores
            tops.append(jnp.maximum(scores[:, :BLK], scores[:, BLK:]))
        top = jnp.maximum(top, jnp.max(functools.reduce(jnp.maximum, tops), axis=1, keepdims=True))
        top_ref[...] = jnp.broadcast_to(top, top_ref.shape)

    def finish(which, local, buffer):
        score_ref, top_ref, stat_ref = buffer
        mixed = weight_stage(score_ref, top_ref, [columns[which % depth, k, BLK:] for k in range(count)])
        weight = jnp.exp2(stat_ref[...] - top_ref[...])
        near_part = jnp.concatenate([ins[2][:, local], ins[6][:, local]], axis=0)
        whole = (mixed[:, :HD] + near_part * weight) / (mixed[:, HD:] + weight)
        for part in range(2):
            outs[part][:, local] = whole[part * part_rows : (part + 1) * part_rows].astype(outs[part].dtype)

    first, second = slice(0, HD), slice(HD, 2 * HD)

    @pl.when(step == 0)
    def _():
        for which in range(3):
            fetch(which)
        arrive(0)
        begin(0, [ins[0][:, first], ins[4][:, first]], buffers[0])

    for offset in (1, 2):
        guarded(arrive, 2 * step + offset)
    for offset in (3, 4):
        guarded(fetch, 2 * step + offset)
    begin(2 * step + 1, [ins[0][:, second], ins[4][:, second]], buffers[1])
    finish(2 * step, first, buffers[0])
    begin(jnp.minimum(2 * step + 2, heads - 1), [ins[1][...], ins[5][...]], buffers[0])
    finish(2 * step + 1, second, buffers[1])


def vertical_half(slots, ok, quarters, queries, near_part, stat, last_z, last_x):
    rows, width = queries.shape
    heads = width // HD
    count = slots.shape[0] // heads
    part = rows // 4
    assert heads % 2 == 0 and heads > 2 and count % 2 == 0
    hbm = pl.BlockSpec(memory_space=pl.ANY)

    def own(which, lanes, column):
        return pl.BlockSpec((part, lanes), lambda t, slot, ok, quarters: (quarters[which], column(t)))

    def mine(which):
        return [
            own(which, 2 * HD, lambda t: t),
            own(which, HD, lambda t: jnp.minimum(2 * t + 2, heads - 1)),
            own(which, 2 * HD, lambda t: t),
            own(which, HD, lambda t: 0),
        ]

    return pl.pallas_call(
        functools.partial(vertical_kernel, count),
        grid_spec=pltpu.PrefetchScalarGridSpec(
            num_scalar_prefetch=3,
            grid=(heads // 2,),
            in_specs=mine(0) + mine(1) + [hbm] * 10,
            out_specs=[pl.BlockSpec((part, 2 * HD), lambda t, *_: (0, t))] * 2,
            scratch_shapes=[pltpu.VMEM((6, count, 2 * BLK, HD), jnp.bfloat16)]
            + [pltpu.VMEM((2 * part, count * BLK), jnp.float32)] * 2
            + [pltpu.VMEM((2 * part, HD), jnp.float32)] * 4
            + [pltpu.SemaphoreType.DMA((6,))],
        ),
        out_shape=[jax.ShapeDtypeStruct((part, width), jnp.bfloat16)] * 2,
        compiler_params=pltpu.CompilerParams(dimension_semantics=("arbitrary",)),
        cost_estimate=cost(2 * part * heads * count, part * width * 32),
        name="vertical",
    )(slots, ok, quarters, *([queries, queries, near_part, stat] * 2), *last_z, *last_x)


def tables(vertical, slash, slab_index, slab_blocks):
    heads, _ = vertical.shape
    blocks = jnp.arange(lax.axis_size(SEQ) * slab_blocks, dtype=jnp.int32)
    flat = vertical.reshape(-1)
    used = jnp.any(flat[:, None] == blocks[None, :], axis=0)
    earlier = (blocks[None, :] // slab_blocks == flat[:, None] // slab_blocks) & (blocks[None, :] < flat[:, None])
    rank = jnp.sum((earlier & used[None, :]).astype(jnp.int32), axis=1)
    slab = flat // slab_blocks
    xs, zs, ys = lax.axis_size("x"), lax.axis_size("z"), lax.axis_size("y")
    dx = (slab // (zs * ys) - lax.axis_index("x")) % xs
    dz = (slab // ys - lax.axis_index("z")) % zs
    half = CAP // 2
    last_x = rank >= half
    piece = jnp.where(last_x, xs * zs + dx * zs + dz, dz * xs + dx)
    slots = (piece * ys + (slab % ys ^ lax.axis_index("y"))) * half + rank % half
    mine = slab_index * slab_blocks + jnp.arange(slab_blocks, dtype=jnp.int32)
    gap = mine[None, :, None] - vertical[:, None, :]
    covered = jnp.any(gap[..., None] == slash[:, None, None, :], axis=3)
    ok = (gap > 0) & jnp.logical_not(covered)
    return slots, ok.astype(jnp.int32).reshape(heads, -1)


def from_ahead(array, axis, by):
    size = lax.axis_size(axis)
    return lax.ppermute(array, axis, [((i + by) % size, i) for i in range(size)])


def along(array, axis):
    return jnp.concatenate([array] + [from_ahead(array, axis, by) for by in (1, 2, 3)], axis=0)


def around(array, axis):
    half = array.shape[0] // 2
    ahead, behind = from_ahead(array, axis, 1), from_ahead(array, axis, 3)
    low, high = from_ahead(ahead[:half], axis, 1), from_ahead(behind[half:], axis, 3)
    return [array, ahead, low, high, behind]


def step(queries, keys, values, vertical, slash):
    slab_blocks = queries.shape[0] // BLK
    parts = lax.axis_size("head")
    slab_index = lax.axis_index(SEQ).astype(jnp.int32)
    base = (slab_index * slab_blocks).reshape(1)
    kv, packed = prep(vertical, base, keys, values)
    slabs = lax.axis_size(SEQ)
    pair = lax.axis_size("y")

    def swapped(array):
        return lax.ppermute(array, "y", [(i, pair - 1 - i) for i in range(pair)])

    def from_before(array, pairs):
        return lax.ppermute(array, SEQ, [(i, (i + pairs * pair) % slabs) for i in range(slabs)])

    half = CAP // 2
    other = swapped(packed)
    last_z = around(along(jnp.concatenate([packed[:half], other[:half]], axis=0), "x"), "z")
    last_x = around(along(jnp.concatenate([packed[half:], other[half:]], axis=0), "z"), "x")
    upper = lax.axis_index("y") == 1
    second, fourth = from_before(kv, 1), from_before(kv, 2)
    first = swapped(jnp.where(upper, second, kv))
    third = swapped(jnp.where(upper, *lax.optimization_barrier((fourth, second))))
    far = fourth[slab_blocks - REACH % slab_blocks :]
    slots, ok = tables(vertical, slash, slab_index, slab_blocks)
    near_part, stat = near(slash, base, queries, far, third, second, first, kv)
    here = lax.axis_index("head").astype(jnp.int32)

    def half(pair):
        quarters = jnp.stack([here ^ step for step in pair])
        return vertical_half(slots, ok, quarters, queries, near_part, stat, last_z, last_x)

    def sent(piece, step):
        return lax.ppermute(piece, "head", [(i, i ^ step) for i in range(parts)])

    second_piece, third_piece = half((2, 3))
    first_piece, own_piece = half((1, 0))
    pieces = [own_piece, sent(first_piece, 1), sent(second_piece, 2), sent(third_piece, 3)]
    width = queries.shape[1]
    out = jnp.zeros((pieces[0].shape[0], width * parts), pieces[0].dtype)
    for step in (0, 1, 2, 3):
        out = lax.dynamic_update_slice_in_dim(out, pieces[step], (here ^ step) * width, 1)
    return out


def solution(mesh):
    split = Mesh(mesh.devices.reshape(mesh.shape["head"], 4, 4, 2), ("head",) + SEQ)
    return jax.shard_map(
        step,
        mesh=split,
        in_specs=(P(SEQ, "head"), P(SEQ, "head"), P(SEQ, "head"), P("head", None), P("head", None)),
        out_specs=P(SEQ + ("head",), None),
        check_vma=False,
    )
```

```python
import functools
import math

import jax
import jax.numpy as jnp
from jax import lax
from jax.experimental import pallas as pl
from jax.experimental.pallas import tpu as pltpu
from jax.sharding import Mesh
from jax.sharding import PartitionSpec as P

BLK = 128
HD = 128
REACH = 28
CAP = 4
NEG = -1e30
SEQ = ("x", "z", "y")
SCALE2 = math.log2(math.e) / math.sqrt(HD)


def cost(row_blocks, moved):
    return pl.CostEstimate(flops=row_blocks * 4 * BLK * HD, bytes_accessed=moved, transcendentals=row_blocks * BLK)


def prep_kernel(vertical_ref, base_ref, keys_ref, values_ref, kv_ref, packed_ref):
    slab_blocks = kv_ref.shape[0]
    base = base_ref[0]

    bits = jnp.int32(0)
    for head in range(vertical_ref.shape[0]):
        for number in range(vertical_ref.shape[1]):
            local = vertical_ref[head, number] - base
            inside = (local >= 0) & (local < slab_blocks)
            bits = bits | jnp.where(inside, 1 << jnp.where(inside, local, 0), 0)
    packed_ref[...] = jnp.zeros(packed_ref.shape, packed_ref.dtype)
    rank = jnp.int32(0)
    for block in range(slab_blocks):
        rows = pl.ds(block * BLK, BLK)
        kv_ref[block, :BLK, :] = keys_ref[rows, :].T
        kv_ref[block, BLK:, :] = values_ref[rows, :]
        used = (bits >> block) & 1

        @pl.when((used == 1) & (rank < CAP))
        def _(block=block, rank=rank):
            packed_ref[rank] = kv_ref[block]

        rank = rank + used


def prep(vertical, base, keys, values):
    slab_blocks = keys.shape[0] // BLK
    whole = lambda shape: pl.BlockSpec(shape, lambda *_: (0,) * len(shape))
    return pl.pallas_call(
        prep_kernel,
        grid_spec=pltpu.PrefetchScalarGridSpec(
            num_scalar_prefetch=2,
            grid=(1,),
            in_specs=[whole(keys.shape), whole(values.shape)],
            out_specs=[whole((slab_blocks, 2 * BLK, HD)), whole((CAP, 2 * BLK, HD))],
        ),
        out_shape=[
            jax.ShapeDtypeStruct((slab_blocks, 2 * BLK, HD), jnp.bfloat16),
            jax.ShapeDtypeStruct((CAP, 2 * BLK, HD), jnp.bfloat16),
        ],
        name="prep",
    )(vertical, base, keys, values)


def bias_columns(flags, rows):
    lanes = lax.broadcasted_iota(jnp.int32, (8, HD), 1)
    columns = jnp.zeros((8, HD), jnp.float32)
    for n, flag in enumerate(flags):
        columns = jnp.where(lanes == n, jnp.where(flag, 0.0, NEG).astype(jnp.float32), columns)
    return jnp.broadcast_to(columns[:1], (rows, HD)).astype(jnp.bfloat16)


def marker_rows(n):
    return (lax.broadcasted_iota(jnp.int32, (HD, BLK), 0) == n).astype(jnp.bfloat16)


def score_stage(q, flags, kts, score_ref, top_ref, causal=None, floor=None):
    left = jnp.concatenate([q, bias_columns(flags, q.shape[0])], axis=1)
    right = jnp.concatenate(
        [jnp.concatenate([kt, marker_rows(n)], axis=0) for n, kt in enumerate(kts)], axis=1
    )
    scores = jnp.dot(left, right, preferred_element_type=jnp.float32)
    parts = [scores[:, n * BLK : (n + 1) * BLK] * SCALE2 for n in range(len(kts))]
    if causal is not None:
        parts[0] = jnp.where(causal, parts[0], NEG)
    for n, part in enumerate(parts):
        score_ref[:, n * BLK : (n + 1) * BLK] = part
    top = jnp.max(functools.reduce(jnp.maximum, parts), axis=1, keepdims=True)
    if floor is not None:
        top = jnp.maximum(top, floor)
    top_ref[...] = jnp.broadcast_to(top, top_ref.shape)


def weight_stage(score_ref, top_ref, vs):
    top = top_ref[...]
    rounded = []
    for n in range(len(vs)):
        weights = jnp.exp2(score_ref[:, n * BLK : (n + 1) * BLK] - top)
        rounded.append(weights.astype(jnp.bfloat16))
    v = jnp.concatenate(vs, axis=0)
    v = jnp.concatenate([v, jnp.ones(v.shape, v.dtype)], axis=1)
    return jnp.dot(jnp.concatenate(rounded, axis=1), v, preferred_element_type=jnp.float32)


def near_kernel(first_head, slash_ref, base_ref, q_ref, next_q_ref, far_ref, third_ref, second_ref, first_ref, own_ref, *refs):
    near_ref, stat_ref, band, score_a, score_b, top_a, top_b, sems = refs[-8:]
    head = first_head + pl.program_id(0)
    last_head = first_head + pl.num_programs(0) - 1
    slab_blocks = own_ref.shape[0]
    slash_count = slash_ref.shape[1]
    lanes = lax.broadcasted_iota(jnp.int32, (BLK, HD), 1)
    causal = lax.broadcasted_iota(jnp.int32, (BLK, BLK), 0) >= lanes
    base = base_ref[0]
    buffers = ((score_a, top_a), (score_b, top_b))

    def offsets_of(which):
        return [slash_ref[which, n] for n in range(slash_count)]

    def places(index, offsets):
        return [index + REACH] + [index + REACH - s for s in offsets]

    def begin(q, index, offsets):
        flags = [True] + [base + index - s >= 0 for s in offsets]
        kts = [band[p, :BLK, :] for p in places(index, offsets)]
        score_stage(q[index * BLK : (index + 1) * BLK, :], flags, kts, *buffers[index % 2], causal=causal)

    def finish(index, offsets):
        rows = slice(index * BLK, (index + 1) * BLK)
        score_ref, top_ref = buffers[index % 2]
        mixed = weight_stage(score_ref, top_ref, [band[p, BLK:, :] for p in places(index, offsets)])
        total = mixed[:, HD:]
        near_ref[rows, :] = mixed[:, :HD] / total
        stat_ref[rows, :] = jnp.where(lanes == head, top_ref[...] + jnp.log2(total), stat_ref[rows, :])

    offsets = offsets_of(head)
    following = offsets_of(jnp.minimum(head + 1, last_head))

    @pl.when(head == first_head)
    def _():
        if first_head:
            stat_ref[...] = refs[1][...]
        start = 0
        copies = []
        far = far_ref.at[pl.ds(slab_blocks - REACH % slab_blocks, REACH % slab_blocks)]
        for number, part in enumerate((far, third_ref, second_ref, first_ref, own_ref)):
            copies.append(pltpu.make_async_copy(part, band.at[pl.ds(start, part.shape[0])], sems.at[number]))
            start += part.shape[0]
        for copy in copies:
            copy.start()
        for copy in copies:
            copy.wait()
        begin(q_ref, 0, offsets)

    for index in range(slab_blocks):
        if index + 1 < slab_blocks:
            begin(q_ref, index + 1, offsets)
        else:
            begin(next_q_ref, 0, following)
        finish(index, offsets)


def near(slash, base, queries, fourth, third, second, first, own, heads, done=()):
    rows, width = queries.shape
    first_head = heads.start
    slab_blocks = rows // BLK
    slash_count = slash.shape[1]
    assert slab_blocks % 2 == 0
    hbm = pl.BlockSpec(memory_space=pl.ANY)
    return pl.pallas_call(
        functools.partial(near_kernel, first_head),
        grid_spec=pltpu.PrefetchScalarGridSpec(
            num_scalar_prefetch=2,
            grid=(len(heads),),
            in_specs=[
                pl.BlockSpec((rows, HD), lambda h, *_: (0, first_head + h)),
                pl.BlockSpec((BLK, HD), lambda h, *_: (0, jnp.minimum(first_head + h + 1, heads.stop - 1))),
            ]
            + [hbm] * 5
            + [hbm, pl.BlockSpec((rows, HD), lambda h, *_: (0, 0))][: len(done)],
            out_specs=[
                pl.BlockSpec((rows, HD), lambda h, *_: (0, first_head + h)),
                pl.BlockSpec((rows, HD), lambda h, *_: (0, 0)),
            ],
            scratch_shapes=[
                pltpu.VMEM((REACH + slab_blocks, 2 * BLK, HD), jnp.bfloat16),
                pltpu.VMEM((BLK, (slash_count + 1) * BLK), jnp.float32),
                pltpu.VMEM((BLK, (slash_count + 1) * BLK), jnp.float32),
                pltpu.VMEM((BLK, HD), jnp.float32),
                pltpu.VMEM((BLK, HD), jnp.float32),
                pltpu.SemaphoreType.DMA((5,)),
            ],
        ),
        out_shape=[
            jax.ShapeDtypeStruct((rows, width), jnp.float32),
            jax.ShapeDtypeStruct((rows, HD), jnp.float32),
        ],
        compiler_params=pltpu.CompilerParams(dimension_semantics=("arbitrary",)),
        input_output_aliases={9: 0} if done else {},
        cost_estimate=cost(rows * len(heads) * (slash_count + 1), rows * width * 4),
        name="near",
    )(slash, base, queries, queries, fourth, third, second, first, own, *done)


def choose(index, options, action):
    if len(options) == 1:
        action(options[0])
        return
    middle = len(options) // 2

    @pl.when(index < middle)
    def _():
        choose(index, options[:middle], action)

    @pl.when(index >= middle)
    def _():
        choose(index - middle, options[middle:], action)


def vertical_kernel(count, quarter_count, piece_count, slot_ref, ok_ref, quarters_ref, *refs):
    ins, refs = refs[: 4 * quarter_count], refs[4 * quarter_count :]
    qs, next_qs, near_parts, stats = (ins[n::4] for n in range(4))
    pieces, refs = refs[:piece_count], refs[piece_count:]
    outs, (columns, score_a, score_b, top_a, top_b, stat_a, stat_b, sems) = refs[:quarter_count], refs[quarter_count:]
    step = pl.program_id(0)
    heads = 2 * pl.num_programs(0)
    depth = columns.shape[0]
    piece = pieces[0].shape[0]
    part_rows = outs[0].shape[0]
    blocks = part_rows // BLK
    lanes = lax.broadcasted_iota(jnp.int32, (quarter_count * part_rows, HD), 1)
    buffers = ((score_a, top_a, stat_a), (score_b, top_b, stat_b))

    def fetch(which):
        place = which % depth
        for k in range(count):
            slot = slot_ref[which * count + k]
            inner = slot % piece

            def take(source, k=k, inner=inner):
                pltpu.make_async_copy(source.at[inner], columns.at[place, k], sems.at[place]).start()

            choose(slot // piece, pieces, take)

    def arrive(which):
        place = which % depth
        pltpu.make_async_copy(columns.at[place], columns.at[place], sems.at[place]).wait()

    def guarded(action, which):
        @pl.when(which < heads)
        def _():
            action(which)

    def begin(which, qs, buffer):
        score_ref, top_ref, stat_ref = buffer
        biases = []
        for part in range(quarter_count):
            for block in range(blocks):
                here = quarters_ref[part] * blocks + block
                flags = [ok_ref[which, here * count + k] > 0 for k in range(count)]
                biases.append(bias_columns(flags, BLK))
        left = jnp.concatenate([jnp.concatenate(qs, axis=0), jnp.concatenate(biases, axis=0)], axis=1)
        stat = jnp.concatenate([stat[...] for stat in stats], axis=0)
        top = jnp.sum(jnp.where(lanes == which, stat, 0.0), axis=1, keepdims=True)
        stat_ref[...] = jnp.broadcast_to(top, stat_ref.shape)
        tops = []
        for k in range(0, count, 2):
            pair = [
                jnp.concatenate([columns[which % depth, n, :BLK], marker_rows(n)], axis=0) for n in (k, k + 1)
            ]
            scores = jnp.dot(left, jnp.concatenate(pair, axis=1), preferred_element_type=jnp.float32) * SCALE2
            score_ref[:, k * BLK : (k + 2) * BLK] = scores
            tops.append(jnp.maximum(scores[:, :BLK], scores[:, BLK:]))
        top = jnp.maximum(top, jnp.max(functools.reduce(jnp.maximum, tops), axis=1, keepdims=True))
        top_ref[...] = jnp.broadcast_to(top, top_ref.shape)

    def finish(which, local, buffer):
        score_ref, top_ref, stat_ref = buffer
        mixed = weight_stage(score_ref, top_ref, [columns[which % depth, k, BLK:] for k in range(count)])
        weight = jnp.exp2(stat_ref[...] - top_ref[...])
        near_part = jnp.concatenate([part[:, local] for part in near_parts], axis=0)
        whole = (mixed[:, :HD] + near_part * weight) / (mixed[:, HD:] + weight)
        for part, out_ref in enumerate(outs):
            out_ref[:, local] = whole[part * part_rows : (part + 1) * part_rows].astype(out_ref.dtype)

    first, second = slice(0, HD), slice(HD, 2 * HD)

    @pl.when(step == 0)
    def _():
        fetch(0)
        arrive(0)
        fetch(1)
        fetch(2)
        begin(0, [q[:, first] for q in qs], buffers[0])

    for offset in (1, 2):
        guarded(arrive, 2 * step + offset)
    for offset in (3, 4):
        guarded(fetch, 2 * step + offset)
    begin(2 * step + 1, [q[:, second] for q in qs], buffers[1])
    finish(2 * step, first, buffers[0])
    begin(jnp.minimum(2 * step + 2, heads - 1), [q[...] for q in next_qs], buffers[0])
    finish(2 * step + 1, second, buffers[1])


def vertical_quarters(slots, ok, quarters, queries, near_part, stat, pieces):
    rows, width = queries.shape
    heads = width // HD
    count = slots.shape[0] // heads
    part = rows // 4
    quarter_count = quarters.shape[0]
    assert heads % 2 == 0 and heads > 2 and count % 2 == 0

    def own(which, lanes, column):
        return pl.BlockSpec((part, lanes), lambda t, slot, ok, quarters: (quarters[which], column(t)))

    def mine(which):
        return [
            own(which, 2 * HD, lambda t: t),
            own(which, HD, lambda t: jnp.minimum(2 * t + 2, heads - 1)),
            own(which, 2 * HD, lambda t: t),
            own(which, HD, lambda t: 0),
        ]

    return pl.pallas_call(
        functools.partial(vertical_kernel, count, quarter_count, len(pieces)),
        grid_spec=pltpu.PrefetchScalarGridSpec(
            num_scalar_prefetch=3,
            grid=(heads // 2,),
            in_specs=[spec for which in range(quarter_count) for spec in mine(which)]
            + [pl.BlockSpec(memory_space=pl.ANY)] * len(pieces),
            out_specs=[pl.BlockSpec((part, 2 * HD), lambda t, *_: (0, t))] * quarter_count,
            scratch_shapes=[pltpu.VMEM((6, count, 2 * BLK, HD), jnp.bfloat16)]
            + [pltpu.VMEM((quarter_count * part, count * BLK), jnp.float32)] * 2
            + [pltpu.VMEM((quarter_count * part, HD), jnp.float32)] * 4
            + [pltpu.SemaphoreType.DMA((6,))],
        ),
        out_shape=[jax.ShapeDtypeStruct((part, width), jnp.bfloat16)] * quarter_count,
        compiler_params=pltpu.CompilerParams(dimension_semantics=("arbitrary",)),
        cost_estimate=cost(quarter_count * part * heads * count, quarter_count * part * width * 16),
        name="vertical",
    )(slots, ok, quarters, *([queries, queries, near_part, stat] * quarter_count), *pieces)


def tables(vertical, slash, slab_index, slab_blocks):
    heads, _ = vertical.shape
    blocks = jnp.arange(lax.axis_size(SEQ) * slab_blocks, dtype=jnp.int32)
    flat = vertical.reshape(-1)
    used = jnp.any(flat[:, None] == blocks[None, :], axis=0)
    earlier = (blocks[None, :] // slab_blocks == flat[:, None] // slab_blocks) & (blocks[None, :] < flat[:, None])
    rank = jnp.sum((earlier & used[None, :]).astype(jnp.int32), axis=1)
    slab = flat // slab_blocks
    xs, zs, ys = lax.axis_size("x"), lax.axis_size("z"), lax.axis_size("y")
    dx = (slab // (zs * ys) - lax.axis_index("x")) % xs
    dz = (slab // ys - lax.axis_index("z")) % zs
    half = CAP // 2
    last_x = rank >= half
    piece = jnp.where(last_x, xs * zs + dx * zs + dz, dz * xs + dx)
    slots = (piece * ys + (slab % ys ^ lax.axis_index("y"))) * half + rank % half
    mine = slab_index * slab_blocks + jnp.arange(slab_blocks, dtype=jnp.int32)
    gap = mine[None, :, None] - vertical[:, None, :]
    covered = jnp.any(gap[..., None] == slash[:, None, None, :], axis=3)
    ok = (gap > 0) & jnp.logical_not(covered)
    return slots, ok.astype(jnp.int32).reshape(heads, -1)


def from_ahead(array, axis, by):
    size = lax.axis_size(axis)
    return lax.ppermute(array, axis, [((i + by) % size, i) for i in range(size)])


def along(array, axis):
    one, two, three = (from_ahead(array, axis, by) for by in (1, 2, 3))
    return jnp.concatenate([array, one], axis=0), jnp.concatenate([two, three], axis=0)


def around(halves, axis):
    ahead, behind = from_ahead(halves[0], axis, 1), from_ahead(halves[1], axis, 3)
    ahead_rest, behind_rest = from_ahead(halves[1], axis, 1), from_ahead(halves[0], axis, 3)
    low, high = from_ahead(ahead, axis, 1), from_ahead(behind, axis, 3)
    return [*halves, ahead, ahead_rest, low, high, behind_rest, behind]


def step(queries, keys, values, vertical, slash):
    slab_blocks = queries.shape[0] // BLK
    parts = lax.axis_size("head")
    slab_index = lax.axis_index(SEQ).astype(jnp.int32)
    base = (slab_index * slab_blocks).reshape(1)
    kv, packed = prep(vertical, base, keys, values)
    slabs = lax.axis_size(SEQ)
    pair = lax.axis_size("y")

    def swapped(array):
        return lax.ppermute(array, "y", [(i, pair - 1 - i) for i in range(pair)])

    def from_before(array, pairs):
        return lax.ppermute(array, SEQ, [(i, (i + pairs * pair) % slabs) for i in range(slabs)])

    half = CAP // 2
    other = swapped(packed)
    over_x = along(jnp.concatenate([packed[:half], other[:half]], axis=0), "x")
    over_z = along(jnp.concatenate([packed[half:], other[half:]], axis=0), "z")
    pieces = around(over_x, "z") + around(over_z, "x")
    upper = lax.axis_index("y") == 1
    second, fourth = from_before(kv, 1), from_before(kv, 2)
    first = swapped(jnp.where(upper, second, kv))
    third = swapped(jnp.where(upper, *lax.optimization_barrier((fourth, second))))
    slots, ok = tables(vertical, slash, slab_index, slab_blocks)
    heads = vertical.shape[0]
    near_args = (slash, base, queries, fourth, third, second, first, kv)
    state = near(*near_args, range(heads // 2))
    near_part, stat = near(*near_args, range(heads // 2, heads), state)
    here = lax.axis_index("head").astype(jnp.int32)

    def done(*steps):
        quarters = jnp.stack([here ^ step for step in steps])
        return vertical_quarters(slots, ok, quarters, queries, near_part, stat, pieces)

    def sent(piece, step):
        return lax.ppermute(piece, "head", [(i, i ^ step) for i in range(parts)])

    second_piece, third_piece = done(2, 3)
    first_piece, own_piece = done(1, 0)
    outs = [own_piece, sent(first_piece, 1), sent(second_piece, 2), sent(third_piece, 3)]
    width = queries.shape[1]
    out = jnp.zeros((own_piece.shape[0], width * parts), own_piece.dtype)
    for step in (0, 1, 2, 3):
        out = lax.dynamic_update_slice_in_dim(out, outs[step], (here ^ step) * width, 1)
    return out


def solution(mesh):
    split = Mesh(mesh.devices.reshape(mesh.shape["head"], 4, 4, 2), ("head",) + SEQ)
    return jax.shard_map(
        step,
        mesh=split,
        in_specs=(P(SEQ, "head"), P(SEQ, "head"), P(SEQ, "head"), P("head", None), P("head", None)),
        out_specs=P(SEQ + ("head",), None),
        check_vma=False,
    )
```

```python
import functools
import math

import jax
import jax.numpy as jnp
from jax import lax
from jax.experimental import pallas as pl
from jax.experimental.pallas import tpu as pltpu
from jax.sharding import Mesh
from jax.sharding import PartitionSpec as P

BLK = 128
HD = 128
REACH = 28
CAP = 4
NEG = -1e30
SEQ = ("x", "z", "y")
SCALE2 = math.log2(math.e) / math.sqrt(HD)


def cost(row_blocks, moved):
    return pl.CostEstimate(flops=row_blocks * 4 * BLK * HD, bytes_accessed=moved, transcendentals=row_blocks * BLK)


def prep_kernel(vertical_ref, base_ref, keys_ref, values_ref, kv_ref, packed_ref):
    slab_blocks = kv_ref.shape[0]
    base = base_ref[0]

    bits = jnp.int32(0)
    for head in range(vertical_ref.shape[0]):
        for number in range(vertical_ref.shape[1]):
            local = vertical_ref[head, number] - base
            inside = (local >= 0) & (local < slab_blocks)
            bits = bits | jnp.where(inside, 1 << jnp.where(inside, local, 0), 0)
    packed_ref[...] = jnp.zeros(packed_ref.shape, packed_ref.dtype)
    rank = jnp.int32(0)
    for block in range(slab_blocks):
        rows = pl.ds(block * BLK, BLK)
        kv_ref[block, :BLK, :] = keys_ref[rows, :].T
        kv_ref[block, BLK:, :] = values_ref[rows, :]
        used = (bits >> block) & 1

        @pl.when((used == 1) & (rank < CAP))
        def _(block=block, rank=rank):
            packed_ref[rank] = kv_ref[block]

        rank = rank + used


def prep(vertical, base, keys, values):
    slab_blocks = keys.shape[0] // BLK
    whole = lambda shape: pl.BlockSpec(shape, lambda *_: (0,) * len(shape))
    return pl.pallas_call(
        prep_kernel,
        grid_spec=pltpu.PrefetchScalarGridSpec(
            num_scalar_prefetch=2,
            grid=(1,),
            in_specs=[whole(keys.shape), whole(values.shape)],
            out_specs=[whole((slab_blocks, 2 * BLK, HD)), whole((CAP, 2 * BLK, HD))],
        ),
        out_shape=[
            jax.ShapeDtypeStruct((slab_blocks, 2 * BLK, HD), jnp.bfloat16),
            jax.ShapeDtypeStruct((CAP, 2 * BLK, HD), jnp.bfloat16),
        ],
        name="prep",
    )(vertical, base, keys, values)


def bias_columns(flags, rows):
    lanes = lax.broadcasted_iota(jnp.int32, (8, HD), 1)
    columns = jnp.zeros((8, HD), jnp.float32)
    for n, flag in enumerate(flags):
        columns = jnp.where(lanes == n, jnp.where(flag, 0.0, NEG).astype(jnp.float32), columns)
    return jnp.broadcast_to(columns[:1], (rows, HD)).astype(jnp.bfloat16)


def marker_rows(n):
    return (lax.broadcasted_iota(jnp.int32, (HD, BLK), 0) == n).astype(jnp.bfloat16)


def score_stage(q, flags, kts, score_ref, top_ref, causal=None, floor=None):
    left = jnp.concatenate([q, bias_columns(flags, q.shape[0])], axis=1)
    right = jnp.concatenate(
        [jnp.concatenate([kt, marker_rows(n)], axis=0) for n, kt in enumerate(kts)], axis=1
    )
    scores = jnp.dot(left, right, preferred_element_type=jnp.float32)
    parts = [scores[:, n * BLK : (n + 1) * BLK] * SCALE2 for n in range(len(kts))]
    if causal is not None:
        parts[0] = jnp.where(causal, parts[0], NEG)
    for n, part in enumerate(parts):
        score_ref[:, n * BLK : (n + 1) * BLK] = part
    top = jnp.max(functools.reduce(jnp.maximum, parts), axis=1, keepdims=True)
    if floor is not None:
        top = jnp.maximum(top, floor)
    top_ref[...] = jnp.broadcast_to(top, top_ref.shape)


def weight_stage(score_ref, top_ref, vs):
    top = top_ref[...]
    rounded = []
    for n in range(len(vs)):
        weights = jnp.exp2(score_ref[:, n * BLK : (n + 1) * BLK] - top)
        rounded.append(weights.astype(jnp.bfloat16))
    v = jnp.concatenate(vs, axis=0)
    v = jnp.concatenate([v, jnp.ones(v.shape, v.dtype)], axis=1)
    return jnp.dot(jnp.concatenate(rounded, axis=1), v, preferred_element_type=jnp.float32)


def near_kernel(first_head, slash_ref, base_ref, q_ref, next_q_ref, far_ref, third_ref, second_ref, first_ref, own_ref, *refs):
    near_ref, stat_ref, band, score_a, score_b, top_a, top_b = refs[-7:]
    head = first_head + pl.program_id(0)
    last_head = first_head + pl.num_programs(0) - 1
    slab_blocks = own_ref.shape[0]
    slash_count = slash_ref.shape[1]
    lanes = lax.broadcasted_iota(jnp.int32, (BLK, HD), 1)
    causal = lax.broadcasted_iota(jnp.int32, (BLK, BLK), 0) >= lanes
    base = base_ref[0]
    buffers = ((score_a, top_a), (score_b, top_b))

    def offsets_of(which):
        return [slash_ref[which, n] for n in range(slash_count)]

    def places(index, offsets):
        return [index + REACH] + [index + REACH - s for s in offsets]

    def begin(q, index, offsets):
        flags = [True] + [base + index - s >= 0 for s in offsets]
        kts = [band[p, :BLK, :] for p in places(index, offsets)]
        score_stage(q[index * BLK : (index + 1) * BLK, :], flags, kts, *buffers[index % 2], causal=causal)

    def finish(index, offsets):
        rows = slice(index * BLK, (index + 1) * BLK)
        score_ref, top_ref = buffers[index % 2]
        mixed = weight_stage(score_ref, top_ref, [band[p, BLK:, :] for p in places(index, offsets)])
        total = mixed[:, HD:]
        near_ref[rows, :] = mixed[:, :HD] / total
        stat_ref[rows, :] = jnp.where(lanes == head, top_ref[...] + jnp.log2(total), stat_ref[rows, :])

    offsets = offsets_of(head)
    following = offsets_of(jnp.minimum(head + 1, last_head))

    @pl.when(head == first_head)
    def _():
        if first_head:
            stat_ref[...] = refs[1][...]
        start = 0
        for part in (far_ref, third_ref, second_ref, first_ref, own_ref):
            skipped = slab_blocks - REACH % slab_blocks if start == 0 else 0
            length = slab_blocks - skipped
            band[start : start + length] = part[skipped:]
            start += length
        begin(q_ref, 0, offsets)

    for index in range(slab_blocks):
        if index + 1 < slab_blocks:
            begin(q_ref, index + 1, offsets)
        else:
            begin(next_q_ref, 0, following)
        finish(index, offsets)


def near(slash, base, queries, fourth, third, second, first, own, heads, done=()):
    rows, width = queries.shape
    first_head = heads.start
    slab_blocks = rows // BLK
    slash_count = slash.shape[1]
    assert slab_blocks % 2 == 0
    hbm = pl.BlockSpec(memory_space=pl.ANY)
    return pl.pallas_call(
        functools.partial(near_kernel, first_head),
        grid_spec=pltpu.PrefetchScalarGridSpec(
            num_scalar_prefetch=2,
            grid=(len(heads),),
            in_specs=[
                pl.BlockSpec((rows, HD), lambda h, *_: (0, first_head + h)),
                pl.BlockSpec((BLK, HD), lambda h, *_: (0, jnp.minimum(first_head + h + 1, heads.stop - 1))),
            ]
            + [pl.BlockSpec(memory_space=pltpu.VMEM)] * 5
            + [hbm, pl.BlockSpec((rows, HD), lambda h, *_: (0, 0))][: len(done)],
            out_specs=[
                pl.BlockSpec((rows, HD), lambda h, *_: (0, first_head + h)),
                pl.BlockSpec((rows, HD), lambda h, *_: (0, 0)),
            ],
            scratch_shapes=[
                pltpu.VMEM((REACH + slab_blocks, 2 * BLK, HD), jnp.bfloat16),
                pltpu.VMEM((BLK, (slash_count + 1) * BLK), jnp.float32),
                pltpu.VMEM((BLK, (slash_count + 1) * BLK), jnp.float32),
                pltpu.VMEM((BLK, HD), jnp.float32),
                pltpu.VMEM((BLK, HD), jnp.float32),
            ],
        ),
        out_shape=[
            jax.ShapeDtypeStruct((rows, width), jnp.float32),
            jax.ShapeDtypeStruct((rows, HD), jnp.float32),
        ],
        compiler_params=pltpu.CompilerParams(dimension_semantics=("arbitrary",)),
        input_output_aliases={9: 0} if done else {},
        cost_estimate=cost(rows * len(heads) * (slash_count + 1), rows * width * 4),
        name="near",
    )(slash, base, queries, queries, fourth, third, second, first, own, *done)


def choose(index, options, action):
    if len(options) == 1:
        action(options[0])
        return
    middle = len(options) // 2

    @pl.when(index < middle)
    def _():
        choose(index, options[:middle], action)

    @pl.when(index >= middle)
    def _():
        choose(index - middle, options[middle:], action)


def vertical_kernel(count, quarter_count, piece_count, slot_ref, ok_ref, quarters_ref, *refs):
    ins, refs = refs[: 4 * quarter_count], refs[4 * quarter_count :]
    qs, next_qs, near_parts, stats = (ins[n::4] for n in range(4))
    pieces, refs = refs[:piece_count], refs[piece_count:]
    outs, (columns, score_a, score_b, top_a, top_b, stat_a, stat_b, sems) = refs[:quarter_count], refs[quarter_count:]
    step = pl.program_id(0)
    heads = 2 * pl.num_programs(0)
    depth = columns.shape[0]
    piece = pieces[0].shape[0]
    part_rows = outs[0].shape[0]
    blocks = part_rows // BLK
    lanes = lax.broadcasted_iota(jnp.int32, (quarter_count * part_rows, HD), 1)
    buffers = ((score_a, top_a, stat_a), (score_b, top_b, stat_b))

    def fetch(which):
        place = which % depth
        for k in range(count):
            slot = slot_ref[which * count + k]
            inner = slot % piece

            def take(source, k=k, inner=inner):
                pltpu.make_async_copy(source.at[inner], columns.at[place, k], sems.at[place]).start()

            choose(slot // piece, pieces, take)

    def arrive(which):
        place = which % depth
        pltpu.make_async_copy(columns.at[place], columns.at[place], sems.at[place]).wait()

    def guarded(action, which):
        @pl.when(which < heads)
        def _():
            action(which)

    def begin(which, qs, buffer):
        score_ref, top_ref, stat_ref = buffer
        biases = []
        for part in range(quarter_count):
            for block in range(blocks):
                here = quarters_ref[part] * blocks + block
                flags = [ok_ref[which, here * count + k] > 0 for k in range(count)]
                biases.append(bias_columns(flags, BLK))
        left = jnp.concatenate([jnp.concatenate(qs, axis=0), jnp.concatenate(biases, axis=0)], axis=1)
        stat = jnp.concatenate([stat[...] for stat in stats], axis=0)
        top = jnp.sum(jnp.where(lanes == which, stat, 0.0), axis=1, keepdims=True)
        stat_ref[...] = jnp.broadcast_to(top, stat_ref.shape)
        tops = []
        for k in range(0, count, 2):
            pair = [
                jnp.concatenate([columns[which % depth, n, :BLK], marker_rows(n)], axis=0) for n in (k, k + 1)
            ]
            scores = jnp.dot(left, jnp.concatenate(pair, axis=1), preferred_element_type=jnp.float32) * SCALE2
            score_ref[:, k * BLK : (k + 2) * BLK] = scores
            tops.append(jnp.maximum(scores[:, :BLK], scores[:, BLK:]))
        top = jnp.maximum(top, jnp.max(functools.reduce(jnp.maximum, tops), axis=1, keepdims=True))
        top_ref[...] = jnp.broadcast_to(top, top_ref.shape)

    def finish(which, local, buffer):
        score_ref, top_ref, stat_ref = buffer
        mixed = weight_stage(score_ref, top_ref, [columns[which % depth, k, BLK:] for k in range(count)])
        weight = jnp.exp2(stat_ref[...] - top_ref[...])
        near_part = jnp.concatenate([part[:, local] for part in near_parts], axis=0)
        whole = (mixed[:, :HD] + near_part * weight) / (mixed[:, HD:] + weight)
        for part, out_ref in enumerate(outs):
            out_ref[:, local] = whole[part * part_rows : (part + 1) * part_rows].astype(out_ref.dtype)

    first, second = slice(0, HD), slice(HD, 2 * HD)

    @pl.when(step == 0)
    def _():
        fetch(0)
        arrive(0)
        fetch(1)
        fetch(2)
        begin(0, [q[:, first] for q in qs], buffers[0])

    for offset in (1, 2):
        guarded(arrive, 2 * step + offset)
    for offset in (3, 4):
        guarded(fetch, 2 * step + offset)
    begin(2 * step + 1, [q[:, second] for q in qs], buffers[1])
    finish(2 * step, first, buffers[0])
    begin(jnp.minimum(2 * step + 2, heads - 1), [q[...] for q in next_qs], buffers[0])
    finish(2 * step + 1, second, buffers[1])


def vertical_quarters(slots, ok, quarters, queries, near_part, stat, pieces):
    rows, width = queries.shape
    heads = width // HD
    count = slots.shape[0] // heads
    part = rows // 4
    quarter_count = quarters.shape[0]
    assert heads % 2 == 0 and heads > 2 and count % 2 == 0

    def own(which, lanes, column):
        return pl.BlockSpec((part, lanes), lambda t, slot, ok, quarters: (quarters[which], column(t)))

    def mine(which):
        return [
            own(which, 2 * HD, lambda t: t),
            own(which, HD, lambda t: jnp.minimum(2 * t + 2, heads - 1)),
            own(which, 2 * HD, lambda t: t),
            own(which, HD, lambda t: 0),
        ]

    return pl.pallas_call(
        functools.partial(vertical_kernel, count, quarter_count, len(pieces)),
        grid_spec=pltpu.PrefetchScalarGridSpec(
            num_scalar_prefetch=3,
            grid=(heads // 2,),
            in_specs=[spec for which in range(quarter_count) for spec in mine(which)]
            + [pl.BlockSpec(memory_space=pl.ANY)] * len(pieces),
            out_specs=[pl.BlockSpec((part, 2 * HD), lambda t, *_: (0, t))] * quarter_count,
            scratch_shapes=[pltpu.VMEM((6, count, 2 * BLK, HD), jnp.bfloat16)]
            + [pltpu.VMEM((quarter_count * part, count * BLK), jnp.float32)] * 2
            + [pltpu.VMEM((quarter_count * part, HD), jnp.float32)] * 4
            + [pltpu.SemaphoreType.DMA((6,))],
        ),
        out_shape=[jax.ShapeDtypeStruct((part, width), jnp.bfloat16)] * quarter_count,
        compiler_params=pltpu.CompilerParams(dimension_semantics=("arbitrary",)),
        cost_estimate=cost(quarter_count * part * heads * count, quarter_count * part * width * 16),
        name="vertical",
    )(slots, ok, quarters, *([queries, queries, near_part, stat] * quarter_count), *pieces)


def tables(vertical, slash, slab_index, slab_blocks):
    heads, _ = vertical.shape
    blocks = jnp.arange(lax.axis_size(SEQ) * slab_blocks, dtype=jnp.int32)
    flat = vertical.reshape(-1)
    used = jnp.any(flat[:, None] == blocks[None, :], axis=0)
    earlier = (blocks[None, :] // slab_blocks == flat[:, None] // slab_blocks) & (blocks[None, :] < flat[:, None])
    rank = jnp.sum((earlier & used[None, :]).astype(jnp.int32), axis=1)
    slab = flat // slab_blocks
    xs, zs, ys = lax.axis_size("x"), lax.axis_size("z"), lax.axis_size("y")
    dx = (slab // (zs * ys) - lax.axis_index("x")) % xs
    dz = (slab // ys - lax.axis_index("z")) % zs
    half = CAP // 2
    last_x = rank >= half
    piece = jnp.where(last_x, xs * zs + dx * zs + dz, dz * xs + dx)
    slots = (piece * ys + (slab % ys ^ lax.axis_index("y"))) * half + rank % half
    mine = slab_index * slab_blocks + jnp.arange(slab_blocks, dtype=jnp.int32)
    gap = mine[None, :, None] - vertical[:, None, :]
    covered = jnp.any(gap[..., None] == slash[:, None, None, :], axis=3)
    ok = (gap > 0) & jnp.logical_not(covered)
    return slots, ok.astype(jnp.int32).reshape(heads, -1)


def from_ahead(array, axis, by):
    size = lax.axis_size(axis)
    return lax.ppermute(array, axis, [((i + by) % size, i) for i in range(size)])


def along(array, axis):
    one, two, three = (from_ahead(array, axis, by) for by in (1, 2, 3))
    return jnp.concatenate([array, one], axis=0), jnp.concatenate([two, three], axis=0)


def around(halves, axis):
    ahead, behind = from_ahead(halves[0], axis, 1), from_ahead(halves[1], axis, 3)
    ahead_rest, behind_rest = from_ahead(halves[1], axis, 1), from_ahead(halves[0], axis, 3)
    low, high = from_ahead(ahead, axis, 1), from_ahead(behind, axis, 3)
    return [*halves, ahead, ahead_rest, low, high, behind_rest, behind]


def step(queries, keys, values, vertical, slash):
    slab_blocks = queries.shape[0] // BLK
    parts = lax.axis_size("head")
    slab_index = lax.axis_index(SEQ).astype(jnp.int32)
    base = (slab_index * slab_blocks).reshape(1)
    kv, packed = prep(vertical, base, keys, values)
    slabs = lax.axis_size(SEQ)
    pair = lax.axis_size("y")

    def swapped(array):
        return lax.ppermute(array, "y", [(i, pair - 1 - i) for i in range(pair)])

    def from_before(array, pairs):
        return lax.ppermute(array, SEQ, [(i, (i + pairs * pair) % slabs) for i in range(slabs)])

    half = CAP // 2
    other = swapped(packed)
    over_x = along(jnp.concatenate([packed[:half], other[:half]], axis=0), "x")
    over_z = along(jnp.concatenate([packed[half:], other[half:]], axis=0), "z")
    pieces = around(over_x, "z") + around(over_z, "x")
    upper = lax.axis_index("y") == 1
    second, fourth = from_before(kv, 1), from_before(kv, 2)
    first = swapped(jnp.where(upper, second, kv))
    third = swapped(jnp.where(upper, *lax.optimization_barrier((fourth, second))))
    slots, ok = tables(vertical, slash, slab_index, slab_blocks)
    heads = vertical.shape[0]
    near_args = (slash, base, queries, fourth, third, second, first, kv)
    state = near(*near_args, range(heads // 2))
    near_part, stat = near(*near_args, range(heads // 2, heads), state)
    here = lax.axis_index("head").astype(jnp.int32)

    def done(*steps):
        quarters = jnp.stack([here ^ step for step in steps])
        return vertical_quarters(slots, ok, quarters, queries, near_part, stat, pieces)

    def sent(piece, step):
        return lax.ppermute(piece, "head", [(i, i ^ step) for i in range(parts)])

    second_piece, third_piece = done(2, 3)
    first_piece, own_piece = done(1, 0)
    outs = [own_piece, sent(first_piece, 1), sent(second_piece, 2), sent(third_piece, 3)]
    width = queries.shape[1]
    out = jnp.zeros((own_piece.shape[0], width * parts), own_piece.dtype)
    for step in (0, 1, 2, 3):
        out = lax.dynamic_update_slice_in_dim(out, outs[step], (here ^ step) * width, 1)
    return out


def solution(mesh):
    split = Mesh(mesh.devices.reshape(mesh.shape["head"], 4, 4, 2), ("head",) + SEQ)
    return jax.shard_map(
        step,
        mesh=split,
        in_specs=(P(SEQ, "head"), P(SEQ, "head"), P(SEQ, "head"), P("head", None), P("head", None)),
        out_specs=P(SEQ + ("head",), None),
        check_vma=False,
    )
```
